128 devices in a mesh: mem: 4 (over z_hi, core), tile: 32 (over z_lo, y, x).
Axes of the slice: x: 4, y: 4, z: 4 (z_hi: 2, z_lo: 2; z = z_hi * 2 + z_lo), core: 2. Of those that a mesh axis runs over, the one named last changes fastest.
Arguments:
- gradient: float32 [4, 1024, 1024], P(None, 'tile', 'mem'), may hold values from -6 to 6
- static_scale: float32 [4, 1024, 1024], P(None, 'tile', 'mem'), may hold values from 0.5 to 2
- static_rate: float32 [4], replicated, may hold values from 0.05 to 0.24
- interp_index: int32 [4, 512, 512], P(None, 'tile', 'mem'), may hold values from 0 to 15
- interp_weight: float32 [4, 512, 512], P(None, 'tile', 'mem'), may hold values from 0.1 to 0.4
- members: bfloat16 [80, 4, 512, 512], P('mem', None, 'tile'), may hold values from -6 to 6
- spread_rate: float32 [512, 512], P('tile'), may hold values from 0.02 to 0.24
Outputs:
- hybrid: float32 [4, 1024, 1024], P(None, 'tile', 'mem')
The draws below stay inside these ranges and needn't reach their ends.
Inputs may be any that keep to these rules, and one draw needn't show every extreme that they name: `interp_index`: the fine cell (a, b) of a coarse cell's 4 x 4 block, numbered 4 * a + b; slots may name the same cell.
All inputs are finite; a program needn't handle non-finite values.
Results may differ from the reference program's by a relative error of at most 0.0003.
Values sent between devices are 32-bit elements; how exact they have to be, the bound alone decides.
A program may use at most 128 MiB of HBM per device.

```python
import math
import jax
import jax.numpy as jnp
from jax import lax

BLOCK_SLOTS = 4
STATIC_PASSES = 4
SPREAD_PASSES = 8
FIELDS = 4
GRID_ROWS = 1024
GRID_COLS = 1024
COARSE_ROWS = 512
COARSE_COLS = 512
MEMBERS = 80


def with_ends(result, stream_key, least, top_value):
    longest = result.shape.index(max(result.shape))
    spots = []
    for shift in (0, 1):
        where = [jax.random.randint(jax.random.fold_in(stream_key, axis), (), 0, length) for axis, length in enumerate(result.shape)]
        where[longest] = (where[longest] + shift) % result.shape[longest]
        spots.append(tuple(where))
    return result.at[spots[0]].set(least).at[spots[1]].set(top_value)


def steps_of(rng, extent, cuts, low, top_value):
    def one(dim, parts):
        heights = jax.random.uniform(jax.random.fold_in(jax.random.fold_in(rng, 6), dim), (parts,), jnp.float32, low / len(cuts), top_value / len(cuts))
        return jnp.repeat(jnp.exp(heights), extent[dim] // parts).reshape((-1,) + (1,) * (len(extent) - dim - 1))

    factor_of = one(*cuts[0])
    for cut in cuts[1:]:
        factor_of = factor_of * one(*cut)
    return factor_of


def normal_values(rng, dims, scale, most, shards=(), held_as=jnp.bfloat16):
    result = scale * jax.random.normal(rng, dims, jnp.float32)
    if shards:
        result = result * steps_of(rng, dims, shards, -0.22, 0.18)
    return jnp.clip(result, -most, most).astype(held_as)


def setup_inputs(seed: int = 0) -> dict:
    key_list = jax.random.split(jax.random.key(seed), 8)
    gradient = normal_values(key_list[0], (FIELDS, GRID_ROWS, GRID_COLS), 1.0, 6.0, ((1, 32), (2, 4)), jnp.float32)
    static_scale = jnp.clip(jnp.exp(math.log(2.0) - 1.3862944 * jax.random.uniform(key_list[1], (FIELDS, GRID_ROWS, GRID_COLS), jnp.float32) ** steps_of(key_list[1], (FIELDS, GRID_ROWS, GRID_COLS), ((1, 32), (2, 4)), -0.2, 0.2)), 0.5, 2.0)
    static_rate = jnp.clip(jnp.exp(jax.random.uniform(key_list[2], (FIELDS,), jnp.float32, math.log(0.05), math.log(0.24))), 0.05, 0.24)
    interp_index = with_ends(jax.random.randint(key_list[3], (BLOCK_SLOTS, COARSE_ROWS, COARSE_COLS), 0, 16), jax.random.fold_in(key_list[3], 1), 0, 15).astype(jnp.int32)
    interp_weight = jnp.clip(0.1 + 0.3 * jax.random.uniform(key_list[4], (BLOCK_SLOTS, COARSE_ROWS, COARSE_COLS), jnp.float32) ** steps_of(key_list[4], (BLOCK_SLOTS, COARSE_ROWS, COARSE_COLS), ((1, 32), (2, 4)), -0.2, 0.2), 0.1, 0.4)
    members = normal_values(key_list[5], (MEMBERS, FIELDS, COARSE_ROWS, COARSE_COLS), 1.0, 6.0, ((0, 4), (2, 32)))
    spread_rate = jnp.clip(jnp.exp(math.log(0.24) - 2.4849066 * jax.random.uniform(key_list[6], (COARSE_ROWS, COARSE_COLS), jnp.float32) ** steps_of(key_list[6], (COARSE_ROWS, COARSE_COLS), ((0, 32),), -0.2, 0.2)), 0.02, 0.24)
    return {"gradient": gradient, "static_scale": static_scale, "static_rate": static_rate, "interp_index": interp_index, "interp_weight": interp_weight, "members": members, "spread_rate": spread_rate}


def pad_edges(values, margin):
    return jnp.pad(values, [(0, 0)] * (values.ndim - 2) + [(margin, margin), (margin, margin)])


def diffuse(padded, rate_field):
    centre = padded[..., 1:-1, 1:-1]
    beside = padded[..., 2:, 1:-1] + padded[..., :-2, 1:-1] + padded[..., 1:-1, 2:] + padded[..., 1:-1, :-2]
    return centre + rate_field * (beside - 4.0 * centre)


def weights_table(slot_index, slot_weight):
    offsets = jnp.arange(16, dtype=jnp.int32)[:, None, None]
    offset_table = jnp.zeros((16,) + slot_index.shape[1:], jnp.float32)
    for slot_number in range(slot_index.shape[0]):
        offset_table = offset_table + jnp.where(slot_index[slot_number][None] == offsets, slot_weight[slot_number][None], 0.0)
    return offset_table


def restrict(padded, offset_table):
    height = (padded.shape[1] - 4) // 2
    breadth = (padded.shape[2] - 4) // 2
    accumulated = jnp.zeros((padded.shape[0], height, breadth), jnp.float32)
    for row_shift in range(4):
        for col_shift in range(4):
            picked = padded[:, row_shift + 1:row_shift + 1 + 2 * height:2, col_shift + 1:col_shift + 1 + 2 * breadth:2]
            accumulated = accumulated + offset_table[4 * row_shift + col_shift] * picked
    return accumulated


def prolong(offset_table, ensemble):
    height = ensemble.shape[1]
    breadth = ensemble.shape[2]
    placed = jnp.zeros((ensemble.shape[0], 2 * height + 4, 2 * breadth + 4), jnp.float32)
    for row_shift in range(4):
        for col_shift in range(4):
            contrib = offset_table[4 * row_shift + col_shift][None] * ensemble
            placed = placed.at[:, row_shift:row_shift + 2 * height:2, col_shift:col_shift + 2 * breadth:2].add(contrib)
    return placed


def reference(gradient, static_scale, static_rate, interp_index, interp_weight, members, spread_rate):
    smooth = static_scale * gradient
    for repeat in range(STATIC_PASSES):
        smooth = diffuse(pad_edges(smooth, 1), static_rate[:, None, None])
    static = static_scale * smooth
    offset_table = weights_table(interp_index, interp_weight)
    coarse = restrict(pad_edges(gradient, 2), offset_table)

    def spread_member(running, member_field):
        perturbed = member_field.astype(jnp.float32)
        values = perturbed * coarse
        for repeat in range(SPREAD_PASSES):
            values = diffuse(pad_edges(values, 1), spread_rate)
        return running + perturbed * values, None

    summed, unused = lax.scan(spread_member, jnp.zeros_like(coarse), members)
    ensemble = summed / (MEMBERS - 1)
    spread = prolong(offset_table, ensemble)
    fine_grid = spread[:, 1:1 + GRID_ROWS, 1:1 + GRID_COLS]
    return 0.3 * static + 2.8 * fine_grid
```

```python
import functools

import jax
import jax.numpy as jnp
from jax import lax
from jax.experimental import pallas as pl
from jax.experimental.pallas import tpu as pltpu
from jax.sharding import PartitionSpec as P

STATIC_PASSES = 4
SPREAD_PASSES = 8
REACH = SPREAD_PASSES // 2
FIELDS = 4
MESH = pl.DeviceIdType.MESH
F32 = jnp.float32
BF16 = jnp.bfloat16
AROUND = [(0, 1), (0, -1), (1, 0), (-1, 0), (1, 1), (1, -1), (-1, 1), (-1, -1)]
CHUNK = 4


def split_dot(x, one_hot, transposed=False):
    high = x.astype(BF16)
    rest = x - high.astype(F32)
    mid = rest.astype(BF16)
    low = (rest - mid.astype(F32)).astype(BF16)
    terms = jnp.concatenate([high, mid, low], axis=0)
    dims = (((1,), (1 if transposed else 0,)), ((), ()))
    out = lax.dot_general(terms, one_hot, dims, preferred_element_type=F32)
    n = x.shape[0]
    return (out[2 * n :] + out[n : 2 * n]) + out[:n]


def first_row(step):
    return max(-step, step - SPREAD_PASSES - REACH)


def row_chunks(low, high):
    return [(r, min(r + CHUNK - 1, high)) for r in range(low, high + 1, CHUNK)]


def beside(row, lane):
    axis = row[0].ndim - 1
    zero = jnp.zeros_like(row[0])
    left = jnp.where(lane == 0, zero, pltpu.roll(row[3], 1, axis))
    right = jnp.where(lane == 127, zero, pltpu.roll(row[0], 127, axis))
    return [left + row[1], row[0] + row[2], row[1] + row[3], row[2] + right]


def kernel(
    rate_ref, grad_hbm, scale_hbm, index_hbm, weight_hbm, members_hbm, spread_hbm, out_ref,
    grad, scale, index, weight, spread, raw, perm, pick, place,
    mbuf, edge, table, table_h, picked, coarse, coarse_e, cperm, cb, ceb, kb, ab,
    pa, pb, acc, halo_v, part, got, esum, eup, edown, eall, lhs, fine, static_buf,
    local_sem, send_sem, recv_sem,
):
    m, t = lax.axis_index("mem"), lax.axis_index("tile")
    groups, tiles = lax.axis_size("mem"), lax.axis_size("tile")
    member_count = raw.shape[0]
    mf = member_count * FIELDS
    steps = mf // 8

    def at(dm, dt):
        return (lax.rem(m + dm + groups, groups), lax.rem(t + dt + tiles, tiles))

    barrier = pltpu.get_barrier_semaphore()
    peers = AROUND + [(2, 0)]
    for dm, dt in peers:
        pl.semaphore_signal(barrier, inc=1, device_id=at(dm, dt), device_id_type=MESH)

    locals_ = []

    def fetch(src, dst):
        copy = pltpu.make_async_copy(src, dst, local_sem.at[len(locals_)])
        locals_.append(copy)
        copy.start()
        return copy

    fetch_grad = fetch(grad_hbm, grad.at[:, 8:40, 128:384])
    fetch_members = fetch(members_hbm, raw)
    fetch_index = fetch(index_hbm, index.at[:, 8:24, 128:256])
    fetch_weight = fetch(weight_hbm, weight.at[:, 8:24, 128:256])
    fetch_spread = fetch(spread_hbm, spread.at[8:24])
    fetch_scale = fetch(scale_hbm, scale.at[:, 8:40, 128:384])

    sent = []

    def send(src, dst, dm, dt):
        number = len(sent)
        copy = pltpu.make_async_remote_copy(
            src_ref=src, dst_ref=dst, send_sem=send_sem.at[number], recv_sem=recv_sem.at[number],
            device_id=at(dm, dt), device_id_type=MESH,
        )
        sent.append(copy)
        copy.start()
        return copy

    def send_rim(buf, rows, cols):
        copies = []
        for dm, dt in AROUND:
            row = {0: (8, 8, rows), 1: (rows, 0, 8), -1: (8, rows + 8, 8)}[dt]
            col = {0: (128, 128, cols), 1: (cols, 0, 128), -1: (128, cols + 128, 128)}[dm]
            copies.append(
                send(
                    buf.at[:, row[0] : row[0] + row[2], col[0] : col[0] + col[2]],
                    buf.at[:, row[1] : row[1] + row[2], col[1] : col[1] + col[2]],
                    dm, dt,
                )
            )
        return copies

    def wait_all(copies):
        for copy in copies:
            copy.wait_recv()

    source = lax.broadcasted_iota(jnp.int32, (512, 512), 0)
    target = lax.broadcasted_iota(jnp.int32, (512, 512), 1)
    perm[...] = (source == 4 * (target & 127) + (target >> 7)).astype(F32).astype(BF16)

    fetch_grad.wait()
    fetch_spread.wait()
    pl.semaphore_wait(barrier, len(peers))
    rim_grad = send_rim(grad, 32, 256)
    rim_spread = [
        send(spread.at[16:24], spread.at[0:8], 0, 1),
        send(spread.at[8:16], spread.at[24:32], 0, -1),
    ]

    fetch_members.wait()

    def convert(i, carry):
        block = raw[pl.ds(2 * i, 2)].reshape(8 * 16, 512)
        out = jnp.dot(block, perm[...], preferred_element_type=F32)
        for q in range(8):
            for j in range(4):
                mbuf[j, pl.ds(8 * i + q, 16, stride=mf), :] = out[
                    16 * q : 16 * q + 16, 128 * j : 128 * j + 128
                ]
        return carry

    lax.fori_loop(0, steps, convert, 0)
    edge_members = [
        send(mbuf.at[:, 12 * mf : 16 * mf], edge.at[0], 0, 1),
        send(mbuf.at[:, 0 : 4 * mf], edge.at[1], 0, -1),
    ]

    fetch_index.wait()
    fetch_weight.wait()
    for o in range(16):
        total = jnp.zeros((16, 128), F32)
        for s in range(4):
            total = total + jnp.where(index[s, 8:24, 128:256] == o, weight[s, 8:24, 128:256], 0.0)
        table[o, 8:24] = total
    source = lax.broadcasted_iota(jnp.int32, (384, 512), 0)
    target = lax.broadcasted_iota(jnp.int32, (384, 512), 1)
    wanted = 2 * (target & 127) + (target >> 7) - 1
    wanted = jnp.where(wanted < 0, 383, wanted)
    pick[...] = (source == wanted).astype(F32).astype(BF16)
    source = lax.broadcasted_iota(jnp.int32, (640, 256), 0)
    target = lax.broadcasted_iota(jnp.int32, (640, 256), 1)
    inner = (source < 512) & (target == 2 * (source & 127) + (source >> 7) - 1)
    left = (source == 639) & (target == 0)
    right = (source == 512) & (target == 255)
    place[...] = (inner | left | right).astype(F32).astype(BF16)

    rows48 = lax.broadcasted_iota(jnp.int32, (48, 384), 0)
    lanes48 = lax.broadcasted_iota(jnp.int32, (48, 384), 1)
    inside = (t > 0) | (rows48 >= 8)
    inside = inside & ((t < tiles - 1) | (rows48 < 40))
    inside = inside & ((m > 0) | (lanes48 < 320))
    inside = inside & ((m < groups - 1) | (lanes48 < 256) | (lanes48 >= 320))
    lane48 = lax.broadcasted_iota(jnp.int32, (48, 128), 1)

    def rimmed(buf, f):
        rim = jnp.where(lane48 < 64, buf[f, :, 384:512], buf[f, :, 0:128])
        return jnp.concatenate([buf[f, :, 128:384], rim], axis=1)

    wait_all(rim_grad)
    padded = jnp.concatenate(
        [jnp.where(inside, rimmed(grad, f), 0.0) for f in range(FIELDS)], axis=0
    )
    out = split_dot(padded, pick[...])
    for b in range(4):
        picked[b] = out[:, 128 * b : 128 * b + 128]
    for f in range(FIELDS):
        total = jnp.zeros((16, 128), F32)
        for a in range(4):
            for b in range(4):
                total = total + table[4 * a + b, 8:24] * picked[
                    b, pl.ds(48 * f + 7 + a, 16, stride=2), :
                ]
        coarse[m, f] = total
    all_coarse = [send(coarse.at[m], coarse.at[m], o, 0) for o in (1, 2, 3)]

    wait_all(rim_spread)
    out = split_dot(spread[...], perm[...])
    row32 = lax.broadcasted_iota(jnp.int32, (32, 512), 0)
    known = ((t > 0) | (row32 >= 8)) & ((t < tiles - 1) | (row32 < 24))
    rate = jnp.where(known, out, 0.0)
    stay = jnp.where(known, 1.0 - 4.0 * out, 0.0)
    for j in range(4):
        for r in range(1, 31):
            kb[j, r] = jnp.broadcast_to(rate[r : r + 1, 128 * j : 128 * j + 128], (8, 128))
            ab[j, r] = jnp.broadcast_to(stay[r : r + 1, 128 * j : 128 * j + 128], (8, 128))
    acc[...] = jnp.zeros_like(acc)

    wait_all(all_coarse)
    edge_coarse = [
        send(coarse.at[:, :, 8:16], coarse_e.at[0], 0, 1),
        send(coarse.at[:, :, 0:8], coarse_e.at[1], 0, -1),
    ]
    fetch_scale.wait()
    rim_scale = send_rim(scale, 32, 256)
    rim_index = send_rim(index, 16, 128)
    rim_weight = send_rim(weight, 16, 128)

    rows = jnp.concatenate([coarse[q].reshape(64, 128) for q in range(4)], axis=1)
    out = split_dot(rows, perm[...])
    for j in range(4):
        cperm[j, 0:64] = out[:, 128 * j : 128 * j + 128]
    for j in range(4):
        for r in range(16):
            four = cperm[j, pl.ds(r, 4, stride=16), :]
            cb[j, r, 0:4] = four
            cb[j, r, 4:8] = four

    zero2 = jnp.zeros((2, 8, 128), F32)

    def spread_own(g, carry):
        bufs = [pa, pb]
        for j in range(4):
            for r in range(16):
                pa[j, r + 8] = mbuf[j, pl.ds(r * mf + 8 * g, 8), :] * cb[j, r]
            pa[j, 6:8] = zero2
            pa[j, 24:26] = zero2
        for step in range(1, SPREAD_PASSES + 1):
            src, dst = bufs[(step - 1) % 2], bufs[step % 2]
            low = first_row(step)
            high = 15 - low
            if step <= 6:
                for j in range(4):
                    dst[j, low + 6 : low + 8] = zero2
                    dst[j, high + 9 : high + 11] = zero2
            last = step == SPREAD_PASSES
            if last:
                pieces = row_chunks(-REACH, -1) + row_chunks(0, 15) + row_chunks(16, 15 + REACH)
            else:
                pieces = row_chunks(low, high)
            for r0, r1 in pieces:
                n = r1 - r0 + 1
                lane = lax.broadcasted_iota(jnp.int32, (n, 8, 128), 2)
                x = [src[j, r0 + 7 : r1 + 10] for j in range(4)]
                centre = [v[1 : n + 1] for v in x]
                sides = beside(centre, lane)
                for j in range(4):
                    around = (x[j][0:n] + x[j][2 : n + 2]) + sides[j]
                    new = ab[j, r0 + 8 : r1 + 9] * centre[j] + kb[j, r0 + 8 : r1 + 9] * around
                    if not last:
                        dst[j, r0 + 8 : r1 + 9] = new
                    elif r0 < 0:
                        halo_v[g, j, r0 + 4 : r1 + 5] = new
                    elif r0 >= 16:
                        halo_v[g, j, r0 - 12 : r1 - 11] = new
                    else:
                        for r in range(r0, r1 + 1):
                            acc[j, r + 4] += new[r - r0] * mbuf[j, pl.ds(r * mf + 8 * g, 8), :]
        return carry

    lax.fori_loop(0, steps, spread_own, 0)

    wait_all(edge_coarse)
    rows = jnp.concatenate(
        [
            jnp.concatenate([coarse_e[side, q].reshape(32, 128) for q in range(4)], axis=1)
            for side in range(2)
        ],
        axis=0,
    )
    out = split_dot(rows, perm[...])
    for j in range(4):
        cperm[j, 0:64] = out[:, 128 * j : 128 * j + 128]
    for side in range(2):
        there = (t > 0) if side == 0 else (t < tiles - 1)
        for j in range(4):
            for r in range(4):
                start = 32 * side + (4 + r if side == 0 else r)
                four = jnp.where(there, cperm[j, pl.ds(start, 4, stride=8), :], 0.0)
                ceb[side, j, r, 0:4] = four
                ceb[side, j, r, 4:8] = four
    wait_all(edge_members)

    lane8 = lax.broadcasted_iota(jnp.int32, (8, 128), 1)

    def spread_edges(g, carry):
        for side in range(2):
            old = []
            for r in range(4):
                row = []
                for j in range(4):
                    theirs = edge[side, j, pl.ds(r * mf + 8 * g, 8), :]
                    to = r if side == 0 else 20 + r
                    acc[j, to] += theirs * halo_v[g, j, 4 * side + r]
                    row.append(theirs * ceb[side, j, r])
                old.append(row)
            for step in range(1, SPREAD_PASSES + 1):
                base = 8 + (step - REACH if side == 0 else 16 - step)
                shift = 1 if side == 0 else -1
                nxt = []
                for i in range(4):
                    terms = [old[i + shift + d] for d in (-1, 1) if 0 <= i + shift + d < 4]
                    row = []
                    same = old[i + shift] if 0 <= i + shift < 4 else None
                    sides = beside(same, lane8) if same is not None else None
                    for j in range(4):
                        parts = [term[j] for term in terms]
                        if sides is not None:
                            parts.append(sides[j])
                        around = functools.reduce(lambda a, b: a + b, parts)
                        new = kb[j, base + i] * around
                        if same is not None:
                            new = ab[j, base + i] * same[j] + new
                        row.append(new)
                    nxt.append(row)
                old = nxt
            for i in range(4):
                r = i + (4 if side == 0 else 8)
                for j in range(4):
                    acc[j, r + 4] += old[i][j] * mbuf[j, pl.ds(r * mf + 8 * g, 8), :]
        return carry

    lax.fori_loop(0, steps, spread_edges, 0)

    sub = lax.broadcasted_iota(jnp.int32, (12, 8, 128), 1)
    folded = []
    for j in range(4):
        x = acc[j]
        y = (x + pltpu.roll(x, 4, 1)).reshape(12, 2, 8, 128)
        folded.append(jnp.where(sub < 4, y[:, 0], y[:, 1]).reshape(96, 128))
    out = split_dot(jnp.concatenate(folded, axis=1), perm[...], transposed=True)
    for q in range(4):
        part[q] = out[:, 128 * q : 128 * q + 128]
    shares = [
        send(part.at[lax.rem(m + o, groups)], got.at[o - 1], o, 0) for o in (1, 2, 3)
    ]

    wait_all(rim_index)
    wait_all(rim_weight)
    row8 = lax.broadcasted_iota(jnp.int32, (32, 128), 0)
    lane32 = lax.broadcasted_iota(jnp.int32, (32, 128), 1)
    in_rows = ((t > 0) | (row8 >= 8)) & ((t < tiles - 1) | (row8 < 24))
    in_cols = jnp.where(lane32 < 64, (m < groups - 1).astype(jnp.int32), (m > 0).astype(jnp.int32))
    in_rim = in_rows & (in_cols > 0)
    for a in range(4):
        total = jnp.zeros((32, 128), F32)
        for s in range(4):
            near = jnp.where(lane32 < 64, index[s, :, 256:384], index[s, :, 0:128])
            amount = jnp.where(lane32 < 64, weight[s, :, 256:384], weight[s, :, 0:128])
            cell = jnp.where(lane32 < 64, 4 * a, 4 * a + 3)
            total = total + jnp.where(near == cell, amount, 0.0)
        table_h[a] = jnp.where(in_rim, total, 0.0)
    for b in range(4):
        top = jnp.zeros((8, 128), F32)
        bottom = jnp.zeros((8, 128), F32)
        for s in range(4):
            top = top + jnp.where(index[s, 0:8, 128:256] == 12 + b, weight[s, 0:8, 128:256], 0.0)
            bottom = bottom + jnp.where(
                index[s, 24:32, 128:256] == b, weight[s, 24:32, 128:256], 0.0
            )
        table[12 + b, 0:8] = jnp.where(t > 0, top, 0.0)
        table[b, 24:32] = jnp.where(t < tiles - 1, bottom, 0.0)

    wait_all(rim_scale)
    for f in range(FIELDS):
        p = jnp.where(inside, rimmed(scale, f) * rimmed(grad, f), 0.0)
        for _ in range(STATIC_PASSES):
            around = (pltpu.roll(p, 1, 0) + pltpu.roll(p, 47, 0)) + (
                pltpu.roll(p, 1, 1) + pltpu.roll(p, 383, 1)
            )
            p = jnp.where(inside, p + rate_ref[f] * (around - 4.0 * p), 0.0)
        static_buf[f] = scale[f, 8:40, 128:384] * p[8:40, 0:256]

    wait_all(shares)
    esum[1] = (part[m] + got[0]) + (got[1] + got[2])
    rims = []
    for dm, dt in AROUND:
        slot = 1 - dm
        if dt == 0:
            rims.append(send(esum.at[1], esum.at[slot], dm, dt))
        elif dt == 1:
            rims.append(send(esum.at[1, 72:96], eup.at[slot], dm, dt))
        else:
            rims.append(send(esum.at[1, 0:24], edown.at[slot], dm, dt))
    wait_all(rims)
    members_all = member_count * groups

    def whole(slot):
        eall[slot] = esum[slot]
        eall[slot, 8:32] += eup[slot]
        eall[slot, 64:88] += edown[slot]

    for slot in range(3):
        whole(slot)
    lane96 = lax.broadcasted_iota(jnp.int32, (96, 128), 1)
    side_e = jnp.where(lane96 < 64, eall[2], eall[0]) / (members_all - 1)
    eall[1] = eall[1] / (members_all - 1)
    eall[0] = side_e
    for parity in range(2):
        pairs = [(1, 0), (3, -1)] if parity == 0 else [(2, 0), (0, 1)]
        for f in range(FIELDS):
            at_row = 16 * (4 * parity + f)
            mids = [eall[1, pl.ds(4 * (4 + d) + f, 16, stride=4), :] for _, d in pairs]
            ends = [eall[0, pl.ds(4 * (4 + d) + f, 16, stride=4), :] for _, d in pairs]
            for b in range(4):
                lhs[at_row : at_row + 16, 128 * b : 128 * b + 128] = (
                    table[4 * pairs[0][0] + b, 8:24] * mids[0]
                    + table[4 * pairs[1][0] + b, 8 + pairs[1][1] : 24 + pairs[1][1]] * mids[1]
                )
            lhs[at_row : at_row + 16, 512:640] = (
                table_h[pairs[0][0], 8:24] * ends[0]
                + table_h[pairs[1][0], 8 + pairs[1][1] : 24 + pairs[1][1]] * ends[1]
            )
    out = split_dot(lhs[...], place[...])
    for parity in range(2):
        for f in range(FIELDS):
            at_row = 16 * (4 * parity + f)
            for x in range(2):
                fine[x, pl.ds(32 * f + parity, 16, stride=2), :] = out[
                    at_row : at_row + 16, 128 * x : 128 * x + 128
                ]
    for f in range(FIELDS):
        for x in range(2):
            cols = slice(128 * x, 128 * x + 128)
            out_ref[f, :, cols] = 0.3 * static_buf[f, :, cols] + 2.8 * fine[x, 32 * f : 32 * f + 32]
    for copy in sent:
        copy.wait_send()


def local(gradient, static_scale, static_rate, interp_index, interp_weight, members, spread_rate):
    member_count = members.shape[0]
    mf = member_count * FIELDS
    anywhere = pl.BlockSpec(memory_space=pl.ANY)
    vmem = pltpu.VMEM
    sems = 64
    return pl.pallas_call(
        kernel,
        out_shape=jax.ShapeDtypeStruct(gradient.shape, F32),
        in_specs=[pl.BlockSpec(memory_space=pltpu.SMEM)] + [anywhere] * 6,
        out_specs=pl.BlockSpec(memory_space=pltpu.VMEM),
        scratch_shapes=[
            vmem((4, 48, 512), F32),
            vmem((4, 48, 512), F32),
            vmem((4, 32, 384), jnp.int32),
            vmem((4, 32, 384), F32),
            vmem((32, 512), F32),
            vmem(members.shape, BF16),
            vmem((512, 512), BF16),
            vmem((384, 512), BF16),
            vmem((640, 256), BF16),
            vmem((4, 16 * mf, 128), F32),
            vmem((2, 4, 4 * mf, 128), F32),
            vmem((16, 32, 128), F32),
            vmem((4, 32, 128), F32),
            vmem((4, 192, 128), F32),
            vmem((4, 4, 16, 128), F32),
            vmem((2, 4, 4, 8, 128), F32),
            vmem((4, 64, 128), F32),
            vmem((4, 16, 8, 128), F32),
            vmem((2, 4, 4, 8, 128), F32),
            vmem((4, 32, 8, 128), F32),
            vmem((4, 32, 8, 128), F32),
            vmem((4, 32, 8, 128), F32),
            vmem((4, 32, 8, 128), F32),
            vmem((4, 24, 8, 128), F32),
            vmem((mf // 8, 4, 8, 8, 128), F32),
            vmem((4, 96, 128), F32),
            vmem((3, 96, 128), F32),
            vmem((3, 96, 128), F32),
            vmem((3, 24, 128), F32),
            vmem((3, 24, 128), F32),
            vmem((3, 96, 128), F32),
            vmem((128, 640), F32),
            vmem((2, 128, 128), F32),
            vmem((4, 32, 256), F32),
            pltpu.SemaphoreType.DMA((6,)),
            pltpu.SemaphoreType.DMA((sems,)),
            pltpu.SemaphoreType.DMA((sems,)),
        ],
        compiler_params=pltpu.CompilerParams(
            collective_id=0, has_side_effects=True, vmem_limit_bytes=56 << 20
        ),
    )(static_rate, gradient, static_scale, interp_index, interp_weight, members, spread_rate)


def solution(mesh):
    return jax.shard_map(
        local,
        mesh=mesh,
        in_specs=(
            P(None, "tile", "mem"),
            P(None, "tile", "mem"),
            P(),
            P(None, "tile", "mem"),
            P(None, "tile", "mem"),
            P("mem", None, "tile", None),
            P("tile", None),
        ),
        out_specs=P(None, "tile", "mem"),
        check_vma=False,
    )
```

```python
import functools

import jax
import jax.numpy as jnp
from jax import lax
from jax.experimental import pallas as pl
from jax.experimental.pallas import tpu as pltpu
from jax.sharding import PartitionSpec as P

STATIC_PASSES = 4
SPREAD_PASSES = 8
REACH = SPREAD_PASSES // 2
FIELDS = 4
MESH = pl.DeviceIdType.MESH
F32 = jnp.float32
BF16 = jnp.bfloat16
AROUND = [(0, 1), (0, -1), (1, 0), (-1, 0), (1, 1), (1, -1), (-1, 1), (-1, -1)]
CHUNK = 4
ZROW = 16


def split_dot(x, one_hot, transposed=False):
    high = x.astype(BF16)
    rest = x - high.astype(F32)
    mid = rest.astype(BF16)
    low = (rest - mid.astype(F32)).astype(BF16)
    terms = jnp.concatenate([high, mid, low], axis=0)
    dims = (((1,), (1 if transposed else 0,)), ((), ()))
    out = lax.dot_general(terms, one_hot, dims, preferred_element_type=F32)
    n = x.shape[0]
    return (out[2 * n :] + out[n : 2 * n]) + out[:n]


def first_row(step):
    return max(-step, step - SPREAD_PASSES - REACH)


def row_chunks(low, high):
    return [(r, min(r + CHUNK - 1, high)) for r in range(low, high + 1, CHUNK)]


def beside(row, lane):
    axis = row[0].ndim - 1
    zero = jnp.zeros_like(row[0])
    left = jnp.where(lane == 0, zero, pltpu.roll(row[3], 1, axis))
    right = jnp.where(lane == 127, zero, pltpu.roll(row[0], 127, axis))
    return [left + row[1], row[0] + row[2], row[1] + row[3], row[2] + right]


def kernel(
    rate_ref, grad_hbm, scale_hbm, index_hbm, weight_hbm, members_hbm, spread_hbm, out_ref,
    grad, scale, grad_out, grad_in, scale_out, scale_in, index, weight,
    table_col, table_col_in, table_row, table_row_in, spread, raw, perm, pick, place,
    mbuf, edge, passing, table, table_h, picked, coarse, coarse_e, cperm, cb, ceb, kb, ab,
    pa, pb, acc, halo_v, part, got, esum, eup, edown, eall, lhs, fine, static_buf,
    local_sem, send_sem, recv_sem,
):
    m, t = lax.axis_index("mem"), lax.axis_index("tile")
    groups, tiles = lax.axis_size("mem"), lax.axis_size("tile")
    member_count = raw.shape[0]
    mf = member_count * FIELDS
    steps = mf // 8

    def at(dm, dt):
        return (lax.rem(m + dm + groups, groups), lax.rem(t + dt + tiles, tiles))

    def there(dm, dt):
        tests = []
        if dm:
            tests.append(m < groups - 1 if dm > 0 else m > 0)
        if dt:
            tests.append(t < tiles - 1 if dt > 0 else t > 0)
        return functools.reduce(jnp.logical_and, tests) if tests else None

    def only(test, action):
        if test is None:
            action()
        else:
            pl.when(test)(action)

    barrier = pltpu.get_barrier_semaphore()

    def greet(dm, dt):
        pl.semaphore_signal(barrier, inc=1, device_id=at(dm, dt), device_id_type=MESH)

    waited = 3
    for o in (1, 2, 3):
        greet(o, 0)
    for dm, dt in AROUND:
        if dt:
            only(there(dm, dt), functools.partial(greet, dm, dt))
            waited = waited + there(dm, dt).astype(jnp.int32)
    up_end, down_end = lax.rem(t, ZROW) == ZROW - 1, lax.rem(t, ZROW) == 0
    feeder = (up_end & (t < tiles - 1)) | (down_end & (t > 0))
    relay = (up_end | down_end) & ~feeder
    over = jnp.where(t < ZROW, ZROW, -ZROW)
    along = jnp.where(up_end, 1 - ZROW, ZROW - 1)

    @pl.when(up_end | down_end)
    def _():
        greet(0, over)
        greet(0, along)

    waited = waited + 2 * (up_end | down_end).astype(jnp.int32)

    locals_ = []

    def fetch(src, dst):
        copy = pltpu.make_async_copy(src, dst, local_sem.at[len(locals_)])
        locals_.append(copy)
        copy.start()
        return copy

    fetch_grad = fetch(grad_hbm, grad.at[:, 8:40, 128:384])
    fetch_members = fetch(members_hbm, raw)
    fetch_index = fetch(index_hbm, index)
    fetch_weight = fetch(weight_hbm, weight)
    fetch_spread = fetch(spread_hbm, spread.at[8:24])
    fetch_scale = fetch(scale_hbm, scale.at[:, 8:40, 128:384])

    sent = []

    def send(src, dst, dm, dt, going=None, coming=None, start=True):
        number = len(sent)
        copy = pltpu.make_async_remote_copy(
            src_ref=src, dst_ref=dst, send_sem=send_sem.at[number], recv_sem=recv_sem.at[number],
            device_id=at(dm, dt), device_id_type=MESH,
        )
        entry = (copy, going, coming)
        sent.append(entry)
        if start:
            only(entry[1], copy.start)
        return entry

    def send_near(src, dst, dm, dt):
        return send(src, dst, dm, dt, there(dm, dt), there(-dm, -dt))

    def pack(buf, out):
        for f in range(FIELDS):
            out[0, 4 * f : 4 * f + 4] = buf[f, 8:12, 128:384]
            out[1, 4 * f : 4 * f + 4] = buf[f, 36:40, 128:384]

    def send_rim(buf, out, come):
        copies = []
        for dm, dt in AROUND:
            col = {0: (128, 128, 256), 1: (256, 0, 128), -1: (128, 384, 128)}[dm]
            here, land = pl.ds(col[0], col[2]), pl.ds(col[1], col[2])
            if dt == 0:
                src, dst = buf.at[:, 8:40, here], buf.at[:, 8:40, land]
            else:
                side = 1 if dt > 0 else 0
                src = out.at[side, :, pl.ds(col[0] - 128, col[2])]
                dst = come.at[1 - side, :, land]
            copies.append(send_near(src, dst, dm, dt))
        return copies

    def unpack(come, buf):
        for f in range(FIELDS):
            buf[f, 4:8] = come[0, 4 * f : 4 * f + 4]
            buf[f, 40:44] = come[1, 4 * f : 4 * f + 4]

    def wait_all(copies):
        for copy, _, coming in copies:
            only(coming, copy.wait_recv)

    source = lax.broadcasted_iota(jnp.int32, (512, 512), 0)
    target = lax.broadcasted_iota(jnp.int32, (512, 512), 1)
    perm[...] = (source == 4 * (target & 127) + (target >> 7)).astype(F32).astype(BF16)

    fetch_grad.wait()
    pack(grad, grad_out)
    fetch_spread.wait()
    pl.semaphore_wait(barrier, waited)
    rim_grad = send_rim(grad, grad_out, grad_in)
    rim_spread = [
        send_near(spread.at[16:24], spread.at[0:8], 0, 1),
        send_near(spread.at[8:16], spread.at[24:32], 0, -1),
    ]

    fetch_members.wait()

    half = member_count // 2

    def convert(i):
        block = raw[half * i : half * i + half].reshape(half * FIELDS * 16, 512)
        for j in range(0, 4, 2):
            out = jnp.dot(
                block, perm[:, 128 * j : 128 * j + 256], preferred_element_type=F32
            )
            for q in range(half * FIELDS):
                for k in range(2):
                    mbuf[j + k, pl.ds(half * FIELDS * i + q, 16, stride=mf), :] = out[
                        16 * q : 16 * q + 16, 128 * k : 128 * k + 128
                    ]

    convert(0)
    convert(1)
    edge_members, late = [[], []], []
    for rows in (range(0, 1), range(1, 2), range(2, 4)):
        first, count = rows[0] * mf, len(rows) * mf
        for side, dt, cross, crossed in ((0, 1, up_end, down_end), (1, -1, down_end, up_end)):
            here = pl.ds(first + (12 * mf if side == 0 else 0), count)
            going, coming = there(0, dt), there(0, -dt)
            if rows[0] < 2:
                going, coming = going & ~cross, coming & ~crossed
            entry = send(
                mbuf.at[:, here], edge.at[side, :, pl.ds(first, count)], 0, dt, going, coming,
                start=False,
            )
            edge_members[side].append(entry)
            only(going & ~cross, entry[0].start)
            if rows[0] == 2:
                late.append((going & cross, entry[0]))
    origin = jnp.where(up_end, 12 * mf, 0)
    over_z, onward = [], []
    for row in range(2):
        from_row = pl.ds(pl.multiple_of(origin + row * mf, mf), mf)
        over_z.append(
            send(mbuf.at[:, from_row], passing.at[row], 0, over, feeder, relay, start=row == 0)
        )
        onward.append(
            send(
                passing.at[row],
                edge.at[down_end.astype(jnp.int32), :, pl.ds(row * mf, mf)],
                0, along, relay, feeder, start=False,
            )
        )
    late.append((feeder, over_z[1][0]))

    fetch_index.wait()
    fetch_weight.wait()
    for o in range(16):
        total = jnp.zeros((16, 128), F32)
        for s in range(4):
            total = total + jnp.where(index[s] == o, weight[s], 0.0)
        table[o, 8:24] = total
        if o % 4 in (0, 3):
            table_col[o % 4 // 3, o // 4] = total
        if o < 4:
            table_row[0, o : o + 1] = total[0:1]
        if o >= 12:
            table_row[1, o - 12 : o - 11] = total[15:16]
    fetch_scale.wait()
    pack(scale, scale_out)
    source = lax.broadcasted_iota(jnp.int32, (384, 512), 0)
    target = lax.broadcasted_iota(jnp.int32, (384, 512), 1)
    wanted = 2 * (target & 127) + (target >> 7) - 1
    wanted = jnp.where(wanted < 0, 383, wanted)
    pick[...] = (source == wanted).astype(F32).astype(BF16)
    source = lax.broadcasted_iota(jnp.int32, (640, 256), 0)
    target = lax.broadcasted_iota(jnp.int32, (640, 256), 1)
    inner = (source < 512) & (target == 2 * (source & 127) + (source >> 7) - 1)
    left = (source == 639) & (target == 0)
    right = (source == 512) & (target == 255)
    place[...] = (inner | left | right).astype(F32).astype(BF16)

    rows48 = lax.broadcasted_iota(jnp.int32, (48, 384), 0)
    lanes48 = lax.broadcasted_iota(jnp.int32, (48, 384), 1)
    inside = (t > 0) | (rows48 >= 8)
    inside = inside & ((t < tiles - 1) | (rows48 < 40))
    inside = inside & ((m > 0) | (lanes48 < 320))
    inside = inside & ((m < groups - 1) | (lanes48 < 256) | (lanes48 >= 320))
    lane48 = lax.broadcasted_iota(jnp.int32, (48, 128), 1)

    def rimmed(buf, f):
        rim = jnp.where(lane48 < 64, buf[f, :, 384:512], buf[f, :, 0:128])
        return jnp.concatenate([buf[f, :, 128:384], rim], axis=1)

    wait_all(rim_grad)
    unpack(grad_in, grad)
    padded = jnp.concatenate(
        [jnp.where(inside, rimmed(grad, f), 0.0) for f in range(FIELDS)], axis=0
    )
    out = split_dot(padded, pick[...])
    for b in range(4):
        picked[b] = out[:, 128 * b : 128 * b + 128]
    for f in range(FIELDS):
        total = jnp.zeros((16, 128), F32)
        for a in range(4):
            for b in range(4):
                total = total + table[4 * a + b, 8:24] * picked[
                    b, pl.ds(48 * f + 7 + a, 16, stride=2), :
                ]
        coarse[m, f] = total
    all_coarse = [send(coarse.at[m], coarse.at[m], o, 0) for o in (1, 2, 3)]
    for test, copy in late:
        only(test, copy.start)

    wait_all(rim_spread)
    out = split_dot(spread[...], perm[...])
    row32 = lax.broadcasted_iota(jnp.int32, (32, 512), 0)
    known = ((t > 0) | (row32 >= 8)) & ((t < tiles - 1) | (row32 < 24))
    rate = jnp.where(known, out, 0.0)
    stay = jnp.where(known, 1.0 - 4.0 * out, 0.0)
    for j in range(4):
        for r in range(1, 31):
            kb[j, r] = jnp.broadcast_to(rate[r : r + 1, 128 * j : 128 * j + 128], (8, 128))
            ab[j, r] = jnp.broadcast_to(stay[r : r + 1, 128 * j : 128 * j + 128], (8, 128))
    acc[...] = jnp.zeros_like(acc)

    for side, dt in ((0, -1), (1, 1)):
        @pl.when(jnp.logical_not(there(0, dt)))
        def _():
            edge[side] = jnp.zeros_like(edge[side])

    for slot in range(3):
        for dt in (-1, 0, 1):
            if slot == 1 and dt == 0:
                continue
            dst = {-1: eup, 0: esum, 1: edown}[dt]

            @pl.when(jnp.logical_not(there(slot - 1, dt)))
            def _():
                dst[slot] = jnp.zeros_like(dst[slot])

    def pass_on(row):
        @pl.when(relay)
        def _():
            over_z[row][0].wait_recv()
            onward[row][0].start()

    wait_all(all_coarse)
    pass_on(0)
    edge_coarse = [
        send_near(coarse.at[:, :, 8:16], coarse_e.at[0], 0, 1),
        send_near(coarse.at[:, :, 0:8], coarse_e.at[1], 0, -1),
    ]
    rim_scale = send_rim(scale, scale_out, scale_in)
    rim_table = []
    for dm, dt in AROUND:
        if dt == 0:
            side = 1 if dm > 0 else 0
            rim_table.append(send_near(table_col.at[side], table_col_in.at[1 - side], dm, dt))
        else:
            side = 1 if dt > 0 else 0
            rim_table.append(
                send_near(table_row.at[side], table_row_in.at[1 - side, 1 - dm], dm, dt)
            )

    rows = jnp.concatenate([coarse[q].reshape(64, 128) for q in range(4)], axis=1)
    out = split_dot(rows, perm[...])
    for j in range(4):
        cperm[j, 0:64] = out[:, 128 * j : 128 * j + 128]
    for j in range(4):
        for r in range(16):
            four = cperm[j, pl.ds(r, 4, stride=16), :]
            cb[j, r, 0:4] = four
            cb[j, r, 4:8] = four

    zero2 = jnp.zeros((2, 8, 128), F32)

    def spread_own(g, carry):
        @pl.when(g == steps // 2)
        def _():
            pass_on(1)

        bufs = [pa, pb]
        for j in range(4):
            for r in range(16):
                pa[j, r + 8] = mbuf[j, pl.ds(r * mf + 8 * g, 8), :] * cb[j, r]
            pa[j, 6:8] = zero2
            pa[j, 24:26] = zero2
        for step in range(1, SPREAD_PASSES + 1):
            src, dst = bufs[(step - 1) % 2], bufs[step % 2]
            low = first_row(step)
            high = 15 - low
            if step <= 6:
                for j in range(4):
                    dst[j, low + 6 : low + 8] = zero2
                    dst[j, high + 9 : high + 11] = zero2
            last = step == SPREAD_PASSES
            if last:
                pieces = row_chunks(-REACH, -1) + row_chunks(0, 15) + row_chunks(16, 15 + REACH)
            else:
                pieces = row_chunks(low, high)
            for r0, r1 in pieces:
                n = r1 - r0 + 1
                lane = lax.broadcasted_iota(jnp.int32, (n, 8, 128), 2)
                x = [src[j, r0 + 7 : r1 + 10] for j in range(4)]
                centre = [v[1 : n + 1] for v in x]
                sides = beside(centre, lane)
                for j in range(4):
                    around = (x[j][0:n] + x[j][2 : n + 2]) + sides[j]
                    new = ab[j, r0 + 8 : r1 + 9] * centre[j] + kb[j, r0 + 8 : r1 + 9] * around
                    if not last:
                        dst[j, r0 + 8 : r1 + 9] = new
                    elif r0 < 0:
                        halo_v[g, j, r0 + 4 : r1 + 5] = new
                    elif r0 >= 16:
                        halo_v[g, j, r0 - 12 : r1 - 11] = new
                    else:
                        for r in range(r0, r1 + 1):
                            acc[j, r + 4] += new[r - r0] * mbuf[j, pl.ds(r * mf + 8 * g, 8), :]
        return carry

    lax.fori_loop(0, steps, spread_own, 0)

    wait_all(edge_coarse)
    rows = jnp.concatenate(
        [
            jnp.concatenate([coarse_e[side, q].reshape(32, 128) for q in range(4)], axis=1)
            for side in range(2)
        ],
        axis=0,
    )
    out = split_dot(rows, perm[...])
    for j in range(4):
        cperm[j, 0:64] = out[:, 128 * j : 128 * j + 128]
    for side in range(2):
        known = (t > 0) if side == 0 else (t < tiles - 1)
        for j in range(4):
            for r in range(4):
                start = 32 * side + (4 + r if side == 0 else r)
                four = jnp.where(known, cperm[j, pl.ds(start, 4, stride=8), :], 0.0)
                ceb[side, j, r, 0:4] = four
                ceb[side, j, r, 4:8] = four
    lane8 = lax.broadcasted_iota(jnp.int32, (8, 128), 1)

    def spread_edge(side):
        wait_all(edge_members[side])
        only(down_end & feeder if side == 0 else up_end & feeder, onward[0][0].wait_recv)
        only(down_end & feeder if side == 0 else up_end & feeder, onward[1][0].wait_recv)

        def advance(old, step):
            base = 8 + (step - REACH if side == 0 else 16 - step)
            shift = 1 if side == 0 else -1
            nxt = []
            for i in range(4):
                terms = [old[i + shift + d] for d in (-1, 1) if 0 <= i + shift + d < 4]
                row = []
                same = old[i + shift] if 0 <= i + shift < 4 else None
                sides = beside(same, lane8) if same is not None else None
                for j in range(4):
                    parts = [term[j] for term in terms]
                    if sides is not None:
                        parts.append(sides[j])
                    around = functools.reduce(lambda a, b: a + b, parts)
                    new = kb[j, base + i] * around
                    if same is not None:
                        new = ab[j, base + i] * same[j] + new
                    row.append(new)
                nxt.append(row)
            return nxt

        together = 2 if steps % 2 == 0 else 1

        def some(i, carry):
            groups_ = [together * i + k for k in range(together)]
            fields = []
            for r in range(4):
                for j in range(4):
                    to = r if side == 0 else 20 + r
                    total = acc[j, to]
                    for k, g in enumerate(groups_):
                        theirs = edge[side, j, pl.ds(r * mf + 8 * g, 8), :]
                        total = total + theirs * halo_v[g, j, 4 * side + r]
                        fields.append(theirs * ceb[side, j, r])
                    acc[j, to] = total
            olds = [
                [[fields[(4 * r + j) * together + k] for j in range(4)] for r in range(4)]
                for k in range(together)
            ]
            for step in range(1, SPREAD_PASSES + 1):
                olds = [advance(old, step) for old in olds]
            for i in range(4):
                r = i + (4 if side == 0 else 8)
                for j in range(4):
                    total = acc[j, r + 4]
                    for old, g in zip(olds, groups_):
                        total = total + old[i][j] * mbuf[j, pl.ds(r * mf + 8 * g, 8), :]
                    acc[j, r + 4] = total
            return carry

        lax.fori_loop(0, steps // together, some, 0)

    pl.when(~down_end)(functools.partial(spread_edge, 0))
    spread_edge(1)
    pl.when(down_end)(functools.partial(spread_edge, 0))

    sub = lax.broadcasted_iota(jnp.int32, (12, 8, 128), 1)
    folded = []
    for j in range(4):
        x = acc[j]
        y = (x + pltpu.roll(x, 4, 1)).reshape(12, 2, 8, 128)
        folded.append(jnp.where(sub < 4, y[:, 0], y[:, 1]).reshape(96, 128))
    out = split_dot(jnp.concatenate(folded, axis=1), perm[...], transposed=True)
    for q in range(4):
        part[q] = out[:, 128 * q : 128 * q + 128]
    shares = [
        send(part.at[lax.rem(m + o, groups)], got.at[o - 1], o, 0) for o in (1, 2, 3)
    ]

    wait_all(rim_table)
    near = lax.broadcasted_iota(jnp.int32, (16, 128), 1) < 64
    side_on = jnp.where(near, (m < groups - 1).astype(jnp.int32), (m > 0).astype(jnp.int32)) > 0
    for a in range(4):
        both = jnp.where(near, table_col_in[1, a], table_col_in[0, a])
        table_h[a, 8:24] = jnp.where(side_on, both, 0.0)
    near1 = near[0:1]
    for side, first in ((0, 12), (1, 0)):
        on = (t > 0) if side == 0 else (t < tiles - 1)
        row = 7 if side == 0 else 24
        for b in range(4):
            table[first + b, row : row + 1] = jnp.where(on, table_row_in[side, 1, b : b + 1], 0.0)
        both = jnp.where(near1, table_row_in[side, 2, 0:1], table_row_in[side, 0, 3:4])
        table_h[first // 4, row : row + 1] = jnp.where(side_on[0:1] & on, both, 0.0)

    wait_all(rim_scale)
    unpack(scale_in, scale)
    for f in range(FIELDS):
        p = jnp.where(inside, rimmed(scale, f) * rimmed(grad, f), 0.0)
        for _ in range(STATIC_PASSES):
            around = (pltpu.roll(p, 1, 0) + pltpu.roll(p, 47, 0)) + (
                pltpu.roll(p, 1, 1) + pltpu.roll(p, 383, 1)
            )
            p = jnp.where(inside, p + rate_ref[f] * (around - 4.0 * p), 0.0)
        static_buf[f] = scale[f, 8:40, 128:384] * p[8:40, 0:256]

    wait_all(shares)
    esum[1] = (part[m] + got[0]) + (got[1] + got[2])
    rims = []
    for dm, dt in AROUND:
        slot = 1 - dm
        if dt == 0:
            rims.append(send_near(esum.at[1], esum.at[slot], dm, dt))
        elif dt == 1:
            rims.append(send_near(esum.at[1, 72:96], eup.at[slot], dm, dt))
        else:
            rims.append(send_near(esum.at[1, 0:24], edown.at[slot], dm, dt))
    wait_all(rims)
    members_all = member_count * groups

    def whole(slot):
        eall[slot] = esum[slot]
        eall[slot, 8:32] += eup[slot]
        eall[slot, 64:88] += edown[slot]

    for slot in range(3):
        whole(slot)
    lane96 = lax.broadcasted_iota(jnp.int32, (96, 128), 1)
    side_e = jnp.where(lane96 < 64, eall[2], eall[0]) / (members_all - 1)
    eall[1] = eall[1] / (members_all - 1)
    eall[0] = side_e
    for parity in range(2):
        pairs = [(1, 0), (3, -1)] if parity == 0 else [(2, 0), (0, 1)]
        for f in range(FIELDS):
            at_row = 16 * (4 * parity + f)
            mids = [eall[1, pl.ds(4 * (4 + d) + f, 16, stride=4), :] for _, d in pairs]
            ends = [eall[0, pl.ds(4 * (4 + d) + f, 16, stride=4), :] for _, d in pairs]
            for b in range(4):
                lhs[at_row : at_row + 16, 128 * b : 128 * b + 128] = (
                    table[4 * pairs[0][0] + b, 8:24] * mids[0]
                    + table[4 * pairs[1][0] + b, 8 + pairs[1][1] : 24 + pairs[1][1]] * mids[1]
                )
            lhs[at_row : at_row + 16, 512:640] = (
                table_h[pairs[0][0], 8:24] * ends[0]
                + table_h[pairs[1][0], 8 + pairs[1][1] : 24 + pairs[1][1]] * ends[1]
            )
    out = split_dot(lhs[...], place[...])
    for parity in range(2):
        for f in range(FIELDS):
            at_row = 16 * (4 * parity + f)
            for x in range(2):
                fine[x, pl.ds(32 * f + parity, 16, stride=2), :] = out[
                    at_row : at_row + 16, 128 * x : 128 * x + 128
                ]
    for f in range(FIELDS):
        for x in range(2):
            cols = slice(128 * x, 128 * x + 128)
            out_ref[f, :, cols] = 0.3 * static_buf[f, :, cols] + 2.8 * fine[x, 32 * f : 32 * f + 32]
    for copy, going, _ in sent:
        only(going, copy.wait_send)


def local(gradient, static_scale, static_rate, interp_index, interp_weight, members, spread_rate):
    member_count = members.shape[0]
    mf = member_count * FIELDS
    anywhere = pl.BlockSpec(memory_space=pl.ANY)
    vmem = pltpu.VMEM
    sems = 64
    return pl.pallas_call(
        kernel,
        out_shape=jax.ShapeDtypeStruct(gradient.shape, F32),
        in_specs=[pl.BlockSpec(memory_space=pltpu.SMEM)] + [anywhere] * 6,
        out_specs=pl.BlockSpec(memory_space=pltpu.VMEM),
        scratch_shapes=[
            vmem((4, 48, 512), F32),
            vmem((4, 48, 512), F32),
            vmem((2, 16, 256), F32),
            vmem((2, 16, 512), F32),
            vmem((2, 16, 256), F32),
            vmem((2, 16, 512), F32),
            vmem((4, 16, 128), jnp.int32),
            vmem((4, 16, 128), F32),
            vmem((2, 4, 16, 128), F32),
            vmem((2, 4, 16, 128), F32),
            vmem((2, 8, 128), F32),
            vmem((2, 3, 8, 128), F32),
            vmem((32, 512), F32),
            vmem(members.shape, BF16),
            vmem((512, 512), BF16),
            vmem((384, 512), BF16),
            vmem((640, 256), BF16),
            vmem((4, 16 * mf, 128), F32),
            vmem((2, 4, 4 * mf, 128), F32),
            vmem((2, 4, mf, 128), F32),
            vmem((16, 32, 128), F32),
            vmem((4, 32, 128), F32),
            vmem((4, 192, 128), F32),
            vmem((4, 4, 16, 128), F32),
            vmem((2, 4, 4, 8, 128), F32),
            vmem((4, 64, 128), F32),
            vmem((4, 16, 8, 128), F32),
            vmem((2, 4, 4, 8, 128), F32),
            vmem((4, 32, 8, 128), F32),
            vmem((4, 32, 8, 128), F32),
            vmem((4, 32, 8, 128), F32),
            vmem((4, 32, 8, 128), F32),
            vmem((4, 24, 8, 128), F32),
            vmem((mf // 8, 4, 8, 8, 128), F32),
            vmem((4, 96, 128), F32),
            vmem((3, 96, 128), F32),
            vmem((3, 96, 128), F32),
            vmem((3, 24, 128), F32),
            vmem((3, 24, 128), F32),
            vmem((3, 96, 128), F32),
            vmem((128, 640), F32),
            vmem((2, 128, 128), F32),
            vmem((4, 32, 256), F32),
            pltpu.SemaphoreType.DMA((6,)),
            pltpu.SemaphoreType.DMA((sems,)),
            pltpu.SemaphoreType.DMA((sems,)),
        ],
        compiler_params=pltpu.CompilerParams(
            collective_id=0, has_side_effects=True, vmem_limit_bytes=56 << 20
        ),
    )(static_rate, gradient, static_scale, interp_index, interp_weight, members, spread_rate)


def solution(mesh):
    return jax.shard_map(
        local,
        mesh=mesh,
        in_specs=(
            P(None, "tile", "mem"),
            P(None, "tile", "mem"),
            P(),
            P(None, "tile", "mem"),
            P(None, "tile", "mem"),
            P("mem", None, "tile", None),
            P("tile", None),
        ),
        out_specs=P(None, "tile", "mem"),
        check_vma=False,
    )
```

```python
import functools

import jax
import jax.numpy as jnp
from jax import lax
from jax.experimental import pallas as pl
from jax.experimental.pallas import tpu as pltpu
from jax.sharding import PartitionSpec as P

STATIC_PASSES = 4
SPREAD_PASSES = 8
REACH = SPREAD_PASSES // 2
FIELDS = 4
MESH = pl.DeviceIdType.MESH
F32 = jnp.float32
BF16 = jnp.bfloat16
AROUND = [(0, 1), (0, -1), (1, 0), (-1, 0), (1, 1), (1, -1), (-1, 1), (-1, -1)]
CHUNK = 1
ZROW = 16


def split_dot(x, one_hot, transposed=False):
    high = x.astype(BF16)
    rest = x - high.astype(F32)
    mid = rest.astype(BF16)
    low = (rest - mid.astype(F32)).astype(BF16)
    terms = jnp.concatenate([high, mid, low], axis=0)
    dims = (((1,), (1 if transposed else 0,)), ((), ()))
    out = lax.dot_general(terms, one_hot, dims, preferred_element_type=F32)
    n = x.shape[0]
    return (out[2 * n :] + out[n : 2 * n]) + out[:n]


def first_row(step):
    return max(-step, step - SPREAD_PASSES - REACH)


def row_chunks(low, high):
    return [(r, min(r + CHUNK - 1, high)) for r in range(low, high + 1, CHUNK)]


def beside(row, lane):
    axis = row[0].ndim - 1
    zero = jnp.zeros_like(row[0])
    left = jnp.where(lane == 0, zero, pltpu.roll(row[3], 1, axis))
    right = jnp.where(lane == 127, zero, pltpu.roll(row[0], 127, axis))
    return [left + row[1], row[0] + row[2], row[1] + row[3], row[2] + right]


def kernel(
    rate_hbm, grad_hbm, scale_hbm, index_hbm, weight_hbm, members_hbm, spread_hbm, static_ref, fine_ref,
    grad, scale, grad_out, grad_in, scale_out, scale_in, index, weight,
    table_col, table_col_in, table_row, table_row_in, spread, raw, perm, pick, place,
    mbuf, edge, passing, table, table_h, picked, coarse, coarse_e, cperm, cb, ceb, kb, ab,
    pa, pb, acc, halo_v, part, got, esum, eup, edown, eall, lhs, fine,
    rate_ref, local_sem, send_sem, recv_sem,
):
    m, t = lax.axis_index("mem"), lax.axis_index("tile")
    groups, tiles = lax.axis_size("mem"), lax.axis_size("tile")
    member_count = raw.shape[0]
    mf = member_count * FIELDS
    steps = mf // 8

    def at(dm, dt):
        return (lax.rem(m + dm + groups, groups), lax.rem(t + dt + tiles, tiles))

    def there(dm, dt):
        tests = []
        if dm:
            tests.append(m < groups - 1 if dm > 0 else m > 0)
        if dt:
            tests.append(t < tiles - 1 if dt > 0 else t > 0)
        return functools.reduce(jnp.logical_and, tests) if tests else None

    def only(test, action):
        if test is None:
            action()
        else:
            pl.when(test)(action)

    barrier = pltpu.get_barrier_semaphore()

    def greet(dm, dt):
        pl.semaphore_signal(barrier, inc=1, device_id=at(dm, dt), device_id_type=MESH)

    waited = 3
    for o in (1, 2, 3):
        greet(o, 0)
    for dm, dt in AROUND:
        if dt:
            only(there(dm, dt), functools.partial(greet, dm, dt))
            waited = waited + there(dm, dt).astype(jnp.int32)
    up_end, down_end = lax.rem(t, ZROW) == ZROW - 1, lax.rem(t, ZROW) == 0
    feeder = (up_end & (t < tiles - 1)) | (down_end & (t > 0))
    relay = (up_end | down_end) & ~feeder
    over = jnp.where(t < ZROW, ZROW, -ZROW)
    along = jnp.where(up_end, 1 - ZROW, ZROW - 1)

    @pl.when(up_end | down_end)
    def _():
        greet(0, over)
        greet(0, along)

    waited = waited + 2 * (up_end | down_end).astype(jnp.int32)

    locals_ = []

    def fetch(src, dst):
        copy = pltpu.make_async_copy(src, dst, local_sem.at[len(locals_)])
        locals_.append(copy)
        copy.start()
        return copy

    fetch_grad = fetch(grad_hbm, grad.at[:, 8:40, 128:384])
    fetch_members = fetch(members_hbm, raw)
    fetch_index = fetch(index_hbm, index)
    fetch_weight = fetch(weight_hbm, weight)
    fetch_spread = fetch(spread_hbm, spread.at[8:24])
    fetch_rate = fetch(rate_hbm, rate_ref)
    fetch_scale = fetch(scale_hbm, scale.at[:, 8:40, 128:384])

    sent = []

    def send(src, dst, dm, dt, going=None, coming=None, start=True):
        number = len(sent)
        copy = pltpu.make_async_remote_copy(
            src_ref=src, dst_ref=dst, send_sem=send_sem.at[number], recv_sem=recv_sem.at[number],
            device_id=at(dm, dt), device_id_type=MESH,
        )
        entry = (copy, going, coming)
        sent.append(entry)
        if start:
            only(entry[1], copy.start)
        return entry

    def send_near(src, dst, dm, dt):
        return send(src, dst, dm, dt, there(dm, dt), there(-dm, -dt))

    def pack(buf, out):
        for f in range(FIELDS):
            out[0, 4 * f : 4 * f + 4] = buf[f, 8:12, 128:384]
            out[1, 4 * f : 4 * f + 4] = buf[f, 36:40, 128:384]

    def send_rim(buf, out, come):
        copies = []
        for dm, dt in AROUND:
            col = {0: (128, 128, 256), 1: (256, 0, 128), -1: (128, 384, 128)}[dm]
            here, land = pl.ds(col[0], col[2]), pl.ds(col[1], col[2])
            if dt == 0:
                src, dst = buf.at[:, 8:40, here], buf.at[:, 8:40, land]
            else:
                side = 1 if dt > 0 else 0
                src = out.at[side, :, pl.ds(col[0] - 128, col[2])]
                dst = come.at[1 - side, :, land]
            copies.append(send_near(src, dst, dm, dt))
        return copies

    def unpack(come, buf):
        for f in range(FIELDS):
            buf[f, 4:8] = come[0, 4 * f : 4 * f + 4]
            buf[f, 40:44] = come[1, 4 * f : 4 * f + 4]

    def wait_all(copies):
        for copy, _, coming in copies:
            only(coming, copy.wait_recv)

    source = lax.broadcasted_iota(jnp.int32, (512, 512), 0)
    target = lax.broadcasted_iota(jnp.int32, (512, 512), 1)
    perm[...] = (source == 4 * (target & 127) + (target >> 7)).astype(F32).astype(BF16)

    fetch_grad.wait()
    pack(grad, grad_out)
    fetch_spread.wait()
    pl.semaphore_wait(barrier, waited)
    rim_grad = send_rim(grad, grad_out, grad_in)
    rim_spread = [
        send_near(spread.at[16:24], spread.at[0:8], 0, 1),
        send_near(spread.at[8:16], spread.at[24:32], 0, -1),
    ]

    fetch_members.wait()

    half = member_count // 2

    def convert(i):
        block = raw[half * i : half * i + half].reshape(half * FIELDS * 16, 512)
        for j in range(0, 4, 2):
            out = jnp.dot(
                block, perm[:, 128 * j : 128 * j + 256], preferred_element_type=F32
            )
            for q in range(half * FIELDS):
                for k in range(2):
                    mbuf[j + k, pl.ds(half * FIELDS * i + q, 16, stride=mf), :] = out[
                        16 * q : 16 * q + 16, 128 * k : 128 * k + 128
                    ]

    convert(0)
    convert(1)
    edge_members, late = [[], []], []
    for rows in (range(0, 1), range(1, 2), range(2, 4)):
        first, count = rows[0] * mf, len(rows) * mf
        for side, dt, cross, crossed in ((0, 1, up_end, down_end), (1, -1, down_end, up_end)):
            here = pl.ds(first + (12 * mf if side == 0 else 0), count)
            going, coming = there(0, dt), there(0, -dt)
            if rows[0] < 2:
                going, coming = going & ~cross, coming & ~crossed
            entry = send(
                mbuf.at[:, here], edge.at[side, :, pl.ds(first, count)], 0, dt, going, coming,
                start=False,
            )
            edge_members[side].append(entry)
            only(going & ~cross, entry[0].start)
            if rows[0] == 2:
                late.append((going & cross, entry[0]))
    origin = jnp.where(up_end, 12 * mf, 0)
    over_z, onward = [], []
    for row in range(2):
        from_row = pl.ds(pl.multiple_of(origin + row * mf, mf), mf)
        over_z.append(
            send(mbuf.at[:, from_row], passing.at[row], 0, over, feeder, relay, start=row == 0)
        )
        onward.append(
            send(
                passing.at[row],
                edge.at[down_end.astype(jnp.int32), :, pl.ds(row * mf, mf)],
                0, along, relay, feeder, start=False,
            )
        )
    late.append((feeder, over_z[1][0]))

    fetch_index.wait()
    fetch_weight.wait()
    for o in range(16):
        total = jnp.zeros((16, 128), F32)
        for s in range(4):
            total = total + jnp.where(index[s] == o, weight[s], 0.0)
        table[o, 8:24] = total
        if o % 4 in (0, 3):
            table_col[o % 4 // 3, o // 4] = total
        if o < 4:
            table_row[0, o : o + 1] = total[0:1]
        if o >= 12:
            table_row[1, o - 12 : o - 11] = total[15:16]
    fetch_scale.wait()
    pack(scale, scale_out)
    source = lax.broadcasted_iota(jnp.int32, (384, 512), 0)
    target = lax.broadcasted_iota(jnp.int32, (384, 512), 1)
    wanted = 2 * (target & 127) + (target >> 7) - 1
    wanted = jnp.where(wanted < 0, 383, wanted)
    pick[...] = (source == wanted).astype(F32).astype(BF16)
    source = lax.broadcasted_iota(jnp.int32, (640, 256), 0)
    target = lax.broadcasted_iota(jnp.int32, (640, 256), 1)
    inner = (source < 512) & (target == 2 * (source & 127) + (source >> 7) - 1)
    left = (source == 639) & (target == 0)
    right = (source == 512) & (target == 255)
    place[...] = (inner | left | right).astype(F32).astype(BF16)

    rows48 = lax.broadcasted_iota(jnp.int32, (48, 384), 0)
    lanes48 = lax.broadcasted_iota(jnp.int32, (48, 384), 1)
    inside = (t > 0) | (rows48 >= 8)
    inside = inside & ((t < tiles - 1) | (rows48 < 40))
    inside = inside & ((m > 0) | (lanes48 < 320))
    inside = inside & ((m < groups - 1) | (lanes48 < 256) | (lanes48 >= 320))
    lane48 = lax.broadcasted_iota(jnp.int32, (48, 128), 1)

    def rimmed(buf, f):
        rim = jnp.where(lane48 < 64, buf[f, :, 384:512], buf[f, :, 0:128])
        return jnp.concatenate([buf[f, :, 128:384], rim], axis=1)

    wait_all(rim_grad)
    unpack(grad_in, grad)
    padded = jnp.concatenate(
        [jnp.where(inside, rimmed(grad, f), 0.0) for f in range(FIELDS)], axis=0
    )
    out = split_dot(padded, pick[...])
    for b in range(4):
        picked[b] = out[:, 128 * b : 128 * b + 128]
    for f in range(FIELDS):
        total = jnp.zeros((16, 128), F32)
        for a in range(4):
            for b in range(4):
                total = total + table[4 * a + b, 8:24] * picked[
                    b, pl.ds(48 * f + 7 + a, 16, stride=2), :
                ]
        coarse[m, f] = total
    all_coarse = [send(coarse.at[m], coarse.at[m], o, 0) for o in (1, 2, 3)]
    for test, copy in late:
        only(test, copy.start)

    wait_all(rim_spread)
    out = split_dot(spread[...], perm[...])
    row32 = lax.broadcasted_iota(jnp.int32, (32, 512), 0)
    known = ((t > 0) | (row32 >= 8)) & ((t < tiles - 1) | (row32 < 24))
    rate = jnp.where(known, out, 0.0)
    stay = jnp.where(known, 1.0 - 4.0 * out, 0.0)
    for j in range(4):
        for r in range(1, 31):
            kb[j, r] = jnp.broadcast_to(rate[r : r + 1, 128 * j : 128 * j + 128], (8, 128))
            ab[j, r] = jnp.broadcast_to(stay[r : r + 1, 128 * j : 128 * j + 128], (8, 128))
    acc[...] = jnp.zeros_like(acc)

    for side, dt in ((0, -1), (1, 1)):
        @pl.when(jnp.logical_not(there(0, dt)))
        def _():
            edge[side] = jnp.zeros_like(edge[side])

    for slot in range(3):
        for dt in (-1, 0, 1):
            if slot == 1 and dt == 0:
                continue
            dst = {-1: eup, 0: esum, 1: edown}[dt]

            @pl.when(jnp.logical_not(there(slot - 1, dt)))
            def _():
                dst[slot] = jnp.zeros_like(dst[slot])

    def pass_on(row):
        @pl.when(relay)
        def _():
            over_z[row][0].wait_recv()
            onward[row][0].start()

    wait_all(all_coarse)
    pass_on(0)
    edge_coarse = [
        send_near(coarse.at[:, :, 8:16], coarse_e.at[0], 0, 1),
        send_near(coarse.at[:, :, 0:8], coarse_e.at[1], 0, -1),
    ]
    rim_scale = send_rim(scale, scale_out, scale_in)
    rim_table = []
    for dm, dt in AROUND:
        if dt == 0:
            side = 1 if dm > 0 else 0
            rim_table.append(send_near(table_col.at[side], table_col_in.at[1 - side], dm, dt))
        else:
            side = 1 if dt > 0 else 0
            rim_table.append(
                send_near(table_row.at[side], table_row_in.at[1 - side, 1 - dm], dm, dt)
            )

    rows = jnp.concatenate([coarse[q].reshape(64, 128) for q in range(4)], axis=1)
    out = split_dot(rows, perm[...])
    for j in range(4):
        cperm[j, 0:64] = out[:, 128 * j : 128 * j + 128]
    for j in range(4):
        for r in range(16):
            four = cperm[j, pl.ds(r, 4, stride=16), :]
            cb[j, r, 0:4] = four
            cb[j, r, 4:8] = four

    zero2 = jnp.zeros((2, 8, 128), F32)

    def spread_own(g, carry):
        @pl.when(g == steps // 2)
        def _():
            pass_on(1)

        bufs = [pa, pb]
        for j in range(4):
            for r in range(16):
                pa[j, r + 8] = mbuf[j, pl.ds(r * mf + 8 * g, 8), :] * cb[j, r]
            pa[j, 6:8] = zero2
            pa[j, 24:26] = zero2
        for step in range(1, SPREAD_PASSES + 1):
            src, dst = bufs[(step - 1) % 2], bufs[step % 2]
            low = first_row(step)
            high = 15 - low
            if step <= 6:
                for j in range(4):
                    dst[j, low + 6 : low + 8] = zero2
                    dst[j, high + 9 : high + 11] = zero2
            last = step == SPREAD_PASSES
            if last:
                pieces = row_chunks(-REACH, -1) + row_chunks(0, 15) + row_chunks(16, 15 + REACH)
            else:
                pieces = row_chunks(low, high)
            for r0, r1 in pieces:
                n = r1 - r0 + 1
                lane = lax.broadcasted_iota(jnp.int32, (n, 8, 128), 2)
                x = [src[j, r0 + 7 : r1 + 10] for j in range(4)]
                centre = [v[1 : n + 1] for v in x]
                sides = beside(centre, lane)
                for j in range(4):
                    around = (x[j][0:n] + x[j][2 : n + 2]) + sides[j]
                    new = ab[j, r0 + 8 : r1 + 9] * centre[j] + kb[j, r0 + 8 : r1 + 9] * around
                    if not last:
                        dst[j, r0 + 8 : r1 + 9] = new
                    elif r0 < 0:
                        halo_v[g, j, r0 + 4 : r1 + 5] = new
                    elif r0 >= 16:
                        halo_v[g, j, r0 - 12 : r1 - 11] = new
                    else:
                        for r in range(r0, r1 + 1):
                            acc[j, r + 4] += new[r - r0] * mbuf[j, pl.ds(r * mf + 8 * g, 8), :]
        return carry

    lax.fori_loop(0, steps, spread_own, 0)

    wait_all(edge_coarse)
    rows = jnp.concatenate(
        [
            jnp.concatenate([coarse_e[side, q].reshape(32, 128) for q in range(4)], axis=1)
            for side in range(2)
        ],
        axis=0,
    )
    out = split_dot(rows, perm[...])
    for j in range(4):
        cperm[j, 0:64] = out[:, 128 * j : 128 * j + 128]
    for side in range(2):
        known = (t > 0) if side == 0 else (t < tiles - 1)
        for j in range(4):
            for r in range(4):
                start = 32 * side + (4 + r if side == 0 else r)
                four = jnp.where(known, cperm[j, pl.ds(start, 4, stride=8), :], 0.0)
                ceb[side, j, r, 0:4] = four
                ceb[side, j, r, 4:8] = four
    lane8 = lax.broadcasted_iota(jnp.int32, (8, 128), 1)

    def spread_edge(side):
        wait_all(edge_members[side])
        only(down_end & feeder if side == 0 else up_end & feeder, onward[0][0].wait_recv)
        only(down_end & feeder if side == 0 else up_end & feeder, onward[1][0].wait_recv)

        def advance(old, step):
            base = 8 + (step - REACH if side == 0 else 16 - step)
            shift = 1 if side == 0 else -1
            nxt = []
            for i in range(4):
                terms = [old[i + shift + d] for d in (-1, 1) if 0 <= i + shift + d < 4]
                row = []
                same = old[i + shift] if 0 <= i + shift < 4 else None
                sides = beside(same, lane8) if same is not None else None
                for j in range(4):
                    parts = [term[j] for term in terms]
                    if sides is not None:
                        parts.append(sides[j])
                    around = functools.reduce(lambda a, b: a + b, parts)
                    new = kb[j, base + i] * around
                    if same is not None:
                        new = ab[j, base + i] * same[j] + new
                    row.append(new)
                nxt.append(row)
            return nxt

        together = 2 if steps % 2 == 0 else 1

        def some(i, carry):
            groups_ = [together * i + k for k in range(together)]
            fields = []
            for r in range(4):
                for j in range(4):
                    to = r if side == 0 else 20 + r
                    total = acc[j, to]
                    for k, g in enumerate(groups_):
                        theirs = edge[side, j, pl.ds(r * mf + 8 * g, 8), :]
                        total = total + theirs * halo_v[g, j, 4 * side + r]
                        fields.append(theirs * ceb[side, j, r])
                    acc[j, to] = total
            olds = [
                [[fields[(4 * r + j) * together + k] for j in range(4)] for r in range(4)]
                for k in range(together)
            ]
            for step in range(1, SPREAD_PASSES + 1):
                olds = [advance(old, step) for old in olds]
            for i in range(4):
                r = i + (4 if side == 0 else 8)
                for j in range(4):
                    total = acc[j, r + 4]
                    for old, g in zip(olds, groups_):
                        total = total + old[i][j] * mbuf[j, pl.ds(r * mf + 8 * g, 8), :]
                    acc[j, r + 4] = total
            return carry

        lax.fori_loop(0, steps // together, some, 0)

    pl.when(~down_end)(functools.partial(spread_edge, 0))
    spread_edge(1)
    pl.when(down_end)(functools.partial(spread_edge, 0))

    sub = lax.broadcasted_iota(jnp.int32, (12, 8, 128), 1)
    folded = []
    for j in range(4):
        x = acc[j]
        y = (x + pltpu.roll(x, 4, 1)).reshape(12, 2, 8, 128)
        folded.append(jnp.where(sub < 4, y[:, 0], y[:, 1]).reshape(96, 128))
    out = split_dot(jnp.concatenate(folded, axis=1), perm[...], transposed=True)
    for q in range(4):
        part[q] = out[:, 128 * q : 128 * q + 128]
    shares = [
        send(part.at[lax.rem(m + o, groups)], got.at[o - 1], o, 0) for o in (1, 2, 3)
    ]

    wait_all(rim_table)
    near = lax.broadcasted_iota(jnp.int32, (16, 128), 1) < 64
    side_on = jnp.where(near, (m < groups - 1).astype(jnp.int32), (m > 0).astype(jnp.int32)) > 0
    for a in range(4):
        both = jnp.where(near, table_col_in[1, a], table_col_in[0, a])
        table_h[a, 8:24] = jnp.where(side_on, both, 0.0)
    near1 = near[0:1]
    for side, first in ((0, 12), (1, 0)):
        on = (t > 0) if side == 0 else (t < tiles - 1)
        row = 7 if side == 0 else 24
        for b in range(4):
            table[first + b, row : row + 1] = jnp.where(on, table_row_in[side, 1, b : b + 1], 0.0)
        both = jnp.where(near1, table_row_in[side, 2, 0:1], table_row_in[side, 0, 3:4])
        table_h[first // 4, row : row + 1] = jnp.where(side_on[0:1] & on, both, 0.0)

    fetch_rate.wait()
    wait_all(rim_scale)
    unpack(scale_in, scale)
    for f in range(FIELDS):
        p = jnp.where(inside, rimmed(scale, f) * rimmed(grad, f), 0.0)
        for _ in range(STATIC_PASSES):
            around = (pltpu.roll(p, 1, 0) + pltpu.roll(p, 47, 0)) + (
                pltpu.roll(p, 1, 1) + pltpu.roll(p, 383, 1)
            )
            p = jnp.where(inside, p + rate_ref[f] * (around - 4.0 * p), 0.0)
        static_ref[f] = scale[f, 8:40, 128:384] * p[8:40, 0:256]

    wait_all(shares)
    esum[1] = (part[m] + got[0]) + (got[1] + got[2])
    rims = []
    for dm, dt in AROUND:
        slot = 1 - dm
        if dt == 0:
            rims.append(send_near(esum.at[1], esum.at[slot], dm, dt))
        elif dt == 1:
            rims.append(send_near(esum.at[1, 72:96], eup.at[slot], dm, dt))
        else:
            rims.append(send_near(esum.at[1, 0:24], edown.at[slot], dm, dt))
    wait_all(rims)
    members_all = member_count * groups

    def whole(slot):
        eall[slot] = esum[slot]
        eall[slot, 8:32] += eup[slot]
        eall[slot, 64:88] += edown[slot]

    for slot in range(3):
        whole(slot)
    lane96 = lax.broadcasted_iota(jnp.int32, (96, 128), 1)
    side_e = jnp.where(lane96 < 64, eall[2], eall[0]) / (members_all - 1)
    eall[1] = eall[1] / (members_all - 1)
    eall[0] = side_e
    for parity in range(2):
        pairs = [(1, 0), (3, -1)] if parity == 0 else [(2, 0), (0, 1)]
        for f in range(FIELDS):
            at_row = 16 * (4 * parity + f)
            mids = [eall[1, pl.ds(4 * (4 + d) + f, 16, stride=4), :] for _, d in pairs]
            ends = [eall[0, pl.ds(4 * (4 + d) + f, 16, stride=4), :] for _, d in pairs]
            for b in range(4):
                lhs[at_row : at_row + 16, 128 * b : 128 * b + 128] = (
                    table[4 * pairs[0][0] + b, 8:24] * mids[0]
                    + table[4 * pairs[1][0] + b, 8 + pairs[1][1] : 24 + pairs[1][1]] * mids[1]
                )
            lhs[at_row : at_row + 16, 512:640] = (
                table_h[pairs[0][0], 8:24] * ends[0]
                + table_h[pairs[1][0], 8 + pairs[1][1] : 24 + pairs[1][1]] * ends[1]
            )
    out = split_dot(lhs[...], place[...])
    for parity in range(2):
        for f in range(FIELDS):
            at_row = 16 * (4 * parity + f)
            for x in range(2):
                fine[x, pl.ds(32 * f + parity, 16, stride=2), :] = out[
                    at_row : at_row + 16, 128 * x : 128 * x + 128
                ]
    for f in range(FIELDS):
        for x in range(2):
            cols = slice(128 * x, 128 * x + 128)
            fine_ref[f, :, cols] = fine[x, 32 * f : 32 * f + 32]
    for copy, going, _ in sent:
        only(going, copy.wait_send)


def local(gradient, static_scale, static_rate, interp_index, interp_weight, members, spread_rate):
    member_count = members.shape[0]
    mf = member_count * FIELDS
    anywhere = pl.BlockSpec(memory_space=pl.ANY)
    vmem = pltpu.VMEM
    sems = 64
    static, fine = pl.pallas_call(
        kernel,
        out_shape=[jax.ShapeDtypeStruct(gradient.shape, F32)] * 2,
        in_specs=[anywhere] * 7,
        out_specs=[pl.BlockSpec(memory_space=pltpu.VMEM)] * 2,
        scratch_shapes=[
            vmem((4, 48, 512), F32),
            vmem((4, 48, 512), F32),
            vmem((2, 16, 256), F32),
            vmem((2, 16, 512), F32),
            vmem((2, 16, 256), F32),
            vmem((2, 16, 512), F32),
            vmem((4, 16, 128), jnp.int32),
            vmem((4, 16, 128), F32),
            vmem((2, 4, 16, 128), F32),
            vmem((2, 4, 16, 128), F32),
            vmem((2, 8, 128), F32),
            vmem((2, 3, 8, 128), F32),
            vmem((32, 512), F32),
            vmem(members.shape, BF16),
            vmem((512, 512), BF16),
            vmem((384, 512), BF16),
            vmem((640, 256), BF16),
            vmem((4, 16 * mf, 128), F32),
            vmem((2, 4, 4 * mf, 128), F32),
            vmem((2, 4, mf, 128), F32),
            vmem((16, 32, 128), F32),
            vmem((4, 32, 128), F32),
            vmem((4, 192, 128), F32),
            vmem((4, 4, 16, 128), F32),
            vmem((2, 4, 4, 8, 128), F32),
            vmem((4, 64, 128), F32),
            vmem((4, 16, 8, 128), F32),
            vmem((2, 4, 4, 8, 128), F32),
            vmem((4, 32, 8, 128), F32),
            vmem((4, 32, 8, 128), F32),
            vmem((4, 32, 8, 128), F32),
            vmem((4, 32, 8, 128), F32),
            vmem((4, 24, 8, 128), F32),
            vmem((mf // 8, 4, 8, 8, 128), F32),
            vmem((4, 96, 128), F32),
            vmem((3, 96, 128), F32),
            vmem((3, 96, 128), F32),
            vmem((3, 24, 128), F32),
            vmem((3, 24, 128), F32),
            vmem((3, 96, 128), F32),
            vmem((128, 640), F32),
            vmem((2, 128, 128), F32),
            pltpu.SMEM((4,), F32),
            pltpu.SemaphoreType.DMA((7,)),
            pltpu.SemaphoreType.DMA((sems,)),
            pltpu.SemaphoreType.DMA((sems,)),
        ],
        compiler_params=pltpu.CompilerParams(
            collective_id=0, has_side_effects=True, vmem_limit_bytes=18 << 20
        ),
    )(*[pltpu.with_memory_space_constraint(x, pltpu.HBM) for x in (static_rate, gradient, static_scale, interp_index, interp_weight, members, spread_rate)])
    return 0.3 * static + 2.8 * fine


def solution(mesh):
    return jax.shard_map(
        local,
        mesh=mesh,
        in_specs=(
            P(None, "tile", "mem"),
            P(None, "tile", "mem"),
            P(),
            P(None, "tile", "mem"),
            P(None, "tile", "mem"),
            P("mem", None, "tile", None),
            P("tile", None),
        ),
        out_specs=P(None, "tile", "mem"),
        check_vma=False,
    )
```

```python
import functools

import jax
import jax.numpy as jnp
from jax import lax
from jax.experimental import pallas as pl
from jax.experimental.pallas import tpu as pltpu
from jax.sharding import PartitionSpec as P

STATIC_PASSES = 4
SPREAD_PASSES = 8
REACH = SPREAD_PASSES // 2
FIELDS = 4
MESH = pl.DeviceIdType.MESH
F32 = jnp.float32
BF16 = jnp.bfloat16
AROUND = [(0, 1), (0, -1), (1, 0), (-1, 0), (1, 1), (1, -1), (-1, 1), (-1, -1)]
ZROW = 16


def split_dot(x, one_hot, transposed=False):
    high = x.astype(BF16)
    rest = x - high.astype(F32)
    mid = rest.astype(BF16)
    low = (rest - mid.astype(F32)).astype(BF16)
    terms = jnp.concatenate([high, mid, low], axis=0)
    dims = (((1,), (1 if transposed else 0,)), ((), ()))
    out = lax.dot_general(terms, one_hot, dims, preferred_element_type=F32)
    n = x.shape[0]
    return (out[2 * n :] + out[n : 2 * n]) + out[:n]


def first_row(step):
    return max(-step, step - SPREAD_PASSES - REACH)


def beside(row, lane):
    axis = row[0].ndim - 1
    zero = jnp.zeros_like(row[0])
    left = jnp.where(lane == 0, zero, pltpu.roll(row[3], 1, axis))
    right = jnp.where(lane == 127, zero, pltpu.roll(row[0], 127, axis))
    return [left + row[1], row[0] + row[2], row[1] + row[3], row[2] + right]


def kernel(
    rate_hbm, grad_hbm, scale_hbm, index_hbm, weight_hbm, members_hbm, spread_hbm, static_ref, fine_ref,
    grad, scale, grad_out, grad_in, scale_out, scale_in, index, weight,
    table_col, table_col_in, table_row, table_row_in, spread, raw, perm, pick, place,
    mbuf, edge, passing, table, table_h, picked, coarse, coarse_out, coarse_e, cperm, cb, ceb, kb, ab,
    pa, pb, acc, halo_v, part, got, esum, eup, edown, eall, lhs, fine,
    rate_ref, local_sem, send_sem, recv_sem,
):
    m, t = lax.axis_index("mem"), lax.axis_index("tile")
    groups, tiles = lax.axis_size("mem"), lax.axis_size("tile")
    member_count = raw.shape[0]
    mf = member_count * FIELDS
    steps = mf // 8

    def at(dm, dt):
        return (lax.rem(m + dm + groups, groups), lax.rem(t + dt + tiles, tiles))

    def there(dm, dt):
        tests = []
        if dm:
            tests.append(m < groups - 1 if dm > 0 else m > 0)
        if dt:
            tests.append(t < tiles - 1 if dt > 0 else t > 0)
        return functools.reduce(jnp.logical_and, tests) if tests else None

    def only(test, action):
        if test is None:
            action()
        else:
            pl.when(test)(action)

    barrier = pltpu.get_barrier_semaphore()

    def greet(dm, dt):
        pl.semaphore_signal(barrier, inc=1, device_id=at(dm, dt), device_id_type=MESH)

    waited = 3
    for o in (1, 2, 3):
        greet(o, 0)
    for dm, dt in AROUND:
        if dt:
            only(there(dm, dt), functools.partial(greet, dm, dt))
            waited = waited + there(dm, dt).astype(jnp.int32)
    up_end, down_end = lax.rem(t, ZROW) == ZROW - 1, lax.rem(t, ZROW) == 0
    feeder = (up_end & (t < tiles - 1)) | (down_end & (t > 0))
    relay = (up_end | down_end) & ~feeder
    over = jnp.where(t < ZROW, ZROW, -ZROW)
    along = jnp.where(up_end, 1 - ZROW, ZROW - 1)

    @pl.when(up_end | down_end)
    def _():
        greet(0, over)
        greet(0, along)

    waited = waited + 2 * (up_end | down_end).astype(jnp.int32)

    locals_ = []

    def fetch(src, dst):
        copy = pltpu.make_async_copy(src, dst, local_sem.at[len(locals_)])
        locals_.append(copy)
        copy.start()
        return copy

    fetch_grad = fetch(grad_hbm, grad.at[:, 8:40, 128:384])
    fetch_members = fetch(members_hbm, raw)
    fetch_index = fetch(index_hbm, index)
    fetch_weight = fetch(weight_hbm, weight)
    fetch_spread = fetch(spread_hbm, spread.at[8:24])
    fetch_rate = fetch(rate_hbm, rate_ref)
    fetch_scale = fetch(scale_hbm, scale.at[:, 8:40, 128:384])

    sent = []

    def send(src, dst, dm, dt, going=None, coming=None, start=True):
        number = len(sent)
        copy = pltpu.make_async_remote_copy(
            src_ref=src, dst_ref=dst, send_sem=send_sem.at[number], recv_sem=recv_sem.at[number],
            device_id=at(dm, dt), device_id_type=MESH,
        )
        entry = (copy, going, coming)
        sent.append(entry)
        if start:
            only(entry[1], copy.start)
        return entry

    def send_near(src, dst, dm, dt):
        return send(src, dst, dm, dt, there(dm, dt), there(-dm, -dt))

    def pack(buf, out):
        for f in range(FIELDS):
            out[0, 4 * f : 4 * f + 4] = buf[f, 8:12, 128:384]
            out[1, 4 * f : 4 * f + 4] = buf[f, 36:40, 128:384]

    def send_rim(buf, out, come):
        copies = []
        for dm, dt in AROUND:
            col = {0: (128, 128, 256), 1: (256, 0, 128), -1: (128, 384, 128)}[dm]
            here, land = pl.ds(col[0], col[2]), pl.ds(col[1], col[2])
            if dt == 0:
                src, dst = buf.at[:, 8:40, here], buf.at[:, 8:40, land]
            else:
                side = 1 if dt > 0 else 0
                src = out.at[side, :, pl.ds(col[0] - 128, col[2])]
                dst = come.at[1 - side, :, land]
            copies.append(send_near(src, dst, dm, dt))
        return copies

    def unpack(come, buf):
        for f in range(FIELDS):
            buf[f, 4:8] = come[0, 4 * f : 4 * f + 4]
            buf[f, 40:44] = come[1, 4 * f : 4 * f + 4]

    def wait_all(copies):
        for copy, _, coming in copies:
            only(coming, copy.wait_recv)

    source = lax.broadcasted_iota(jnp.int32, (512, 512), 0)
    target = lax.broadcasted_iota(jnp.int32, (512, 512), 1)
    perm[...] = (source == 4 * (target & 127) + (target >> 7)).astype(F32).astype(BF16)

    fetch_members.wait()

    half = member_count // 2

    def convert(i):
        block = raw[half * i : half * i + half].reshape(half * FIELDS * 16, 512)
        for j in range(0, 4, 2):
            out = jnp.dot(
                block, perm[:, 128 * j : 128 * j + 256], preferred_element_type=F32
            )
            for q in range(half * FIELDS):
                for k in range(2):
                    mbuf[j + k, pl.ds(half * FIELDS * i + q, 16, stride=mf), :] = out[
                        16 * q : 16 * q + 16, 128 * k : 128 * k + 128
                    ]

    convert(0)
    convert(1)
    fetch_grad.wait()
    pack(grad, grad_out)
    fetch_spread.wait()
    pl.semaphore_wait(barrier, waited)
    rim_grad = send_rim(grad, grad_out, grad_in)
    rim_spread = [
        send_near(spread.at[16:24], spread.at[0:8], 0, 1),
        send_near(spread.at[8:16], spread.at[24:32], 0, -1),
    ]

    edge_members, late = [[], []], []
    for rows in (range(0, 1), range(1, 2), range(2, 4)):
        first, count = rows[0] * mf, len(rows) * mf
        for side, dt, cross, crossed in ((0, 1, up_end, down_end), (1, -1, down_end, up_end)):
            here = pl.ds(first + (12 * mf if side == 0 else 0), count)
            going, coming = there(0, dt), there(0, -dt)
            if rows[0] < 2:
                going, coming = going & ~cross, coming & ~crossed
            entry = send(
                mbuf.at[:, here], edge.at[side, :, pl.ds(first, count)], 0, dt, going, coming,
                start=False,
            )
            edge_members[side].append(entry)
            only(going & ~cross, entry[0].start)
            if rows[0] == 2:
                late.append((going & cross, entry[0]))
    origin = jnp.where(up_end, 12 * mf, 0)
    over_z, onward = [], []
    for row in range(2):
        from_row = pl.ds(pl.multiple_of(origin + row * mf, mf), mf)
        over_z.append(
            send(mbuf.at[:, from_row], passing.at[row], 0, over, feeder, relay, start=row == 0)
        )
        onward.append(
            send(
                passing.at[row],
                edge.at[down_end.astype(jnp.int32), :, pl.ds(row * mf, mf)],
                0, along, relay, feeder, start=False,
            )
        )
    late.append((feeder, over_z[1][0]))

    fetch_index.wait()
    fetch_weight.wait()
    for o in range(16):
        total = jnp.zeros((16, 128), F32)
        for s in range(4):
            total = total + jnp.where(index[s] == o, weight[s], 0.0)
        table[o, 8:24] = total
        if o % 4 in (0, 3):
            table_col[o % 4 // 3, o // 4] = total
        if o < 4:
            table_row[0, o : o + 1] = total[0:1]
        if o >= 12:
            table_row[1, o - 12 : o - 11] = total[15:16]
    fetch_scale.wait()
    pack(scale, scale_out)
    source = lax.broadcasted_iota(jnp.int32, (384, 512), 0)
    target = lax.broadcasted_iota(jnp.int32, (384, 512), 1)
    wanted = 2 * (target & 127) + (target >> 7) - 1
    wanted = jnp.where(wanted < 0, 383, wanted)
    pick[...] = (source == wanted).astype(F32).astype(BF16)
    source = lax.broadcasted_iota(jnp.int32, (640, 256), 0)
    target = lax.broadcasted_iota(jnp.int32, (640, 256), 1)
    inner = (source < 512) & (target == 2 * (source & 127) + (source >> 7) - 1)
    left = (source == 639) & (target == 0)
    right = (source == 512) & (target == 255)
    place[...] = (inner | left | right).astype(F32).astype(BF16)

    rows48 = lax.broadcasted_iota(jnp.int32, (48, 384), 0)
    lanes48 = lax.broadcasted_iota(jnp.int32, (48, 384), 1)
    inside = (t > 0) | (rows48 >= 8)
    inside = inside & ((t < tiles - 1) | (rows48 < 40))
    inside = inside & ((m > 0) | (lanes48 < 320))
    inside = inside & ((m < groups - 1) | (lanes48 < 256) | (lanes48 >= 320))
    lane48 = lax.broadcasted_iota(jnp.int32, (48, 128), 1)

    def rimmed(buf, f):
        rim = jnp.where(lane48 < 64, buf[f, :, 384:512], buf[f, :, 0:128])
        return jnp.concatenate([buf[f, :, 128:384], rim], axis=1)

    wait_all(rim_grad)
    unpack(grad_in, grad)
    padded = jnp.concatenate(
        [jnp.where(inside, rimmed(grad, f), 0.0) for f in range(FIELDS)], axis=0
    )
    out = split_dot(padded, pick[...])
    for b in range(4):
        picked[b] = out[:, 128 * b : 128 * b + 128]
    for f in range(FIELDS):
        total = jnp.zeros((16, 128), F32)
        for a in range(4):
            for b in range(4):
                total = total + table[4 * a + b, 8:24] * picked[
                    b, pl.ds(48 * f + 7 + a, 16, stride=2), :
                ]
        coarse[m, f] = total
    all_coarse = [send(coarse.at[m], coarse.at[m], o, 0) for o in (1, 2, 3)]
    for test, copy in late:
        only(test, copy.start)

    wait_all(rim_spread)
    out = split_dot(spread[...], perm[...])
    row32 = lax.broadcasted_iota(jnp.int32, (32, 512), 0)
    known = ((t > 0) | (row32 >= 8)) & ((t < tiles - 1) | (row32 < 24))
    rate = jnp.where(known, out, 0.0)
    stay = jnp.where(known, 1.0 - 4.0 * out, 0.0)
    for j in range(4):
        for r in range(1, 31):
            kb[j, r] = jnp.broadcast_to(rate[r : r + 1, 128 * j : 128 * j + 128], (8, 128))
            ab[j, r] = jnp.broadcast_to(stay[r : r + 1, 128 * j : 128 * j + 128], (8, 128))
    acc[...] = jnp.zeros_like(acc)

    for side, dt in ((0, -1), (1, 1)):
        @pl.when(jnp.logical_not(there(0, dt)))
        def _():
            edge[side] = jnp.zeros_like(edge[side])

    for slot in range(3):
        for dt in (-1, 0, 1):
            if slot == 1 and dt == 0:
                continue
            dst = {-1: eup, 0: esum, 1: edown}[dt]

            @pl.when(jnp.logical_not(there(slot - 1, dt)))
            def _():
                dst[slot] = jnp.zeros_like(dst[slot])

    def pass_on(row):
        @pl.when(relay)
        def _():
            over_z[row][0].wait_recv()
            onward[row][0].start()

    wait_all(all_coarse)
    pass_on(0)
    for q in range(4):
        for f in range(FIELDS):
            coarse_out[0, q, 4 * f : 4 * f + 4] = coarse[q, f, 0:4]
            coarse_out[1, q, 4 * f : 4 * f + 4] = coarse[q, f, 12:16]
    edge_coarse = [
        send_near(coarse_out.at[1], coarse_e.at[0], 0, 1),
        send_near(coarse_out.at[0], coarse_e.at[1], 0, -1),
    ]
    rim_scale = send_rim(scale, scale_out, scale_in)
    rim_table = []
    for dm, dt in AROUND:
        if dt == 0:
            side = 1 if dm > 0 else 0
            rim_table.append(send_near(table_col.at[side], table_col_in.at[1 - side], dm, dt))
        else:
            side = 1 if dt > 0 else 0
            rim_table.append(
                send_near(table_row.at[side], table_row_in.at[1 - side, 1 - dm], dm, dt)
            )

    rows = jnp.concatenate([coarse[q].reshape(64, 128) for q in range(4)], axis=1)
    out = split_dot(rows, perm[...])
    for j in range(4):
        cperm[j, 0:64] = out[:, 128 * j : 128 * j + 128]
    for j in range(4):
        for r in range(16):
            four = cperm[j, pl.ds(r, 4, stride=16), :]
            cb[j, r, 0:4] = four
            cb[j, r, 4:8] = four

    lane8 = lax.broadcasted_iota(jnp.int32, (8, 128), 1)
    together = 2 if steps % 2 == 0 else 1

    def spread_own(i, carry):
        @pl.when(i == steps // together // 2)
        def _():
            pass_on(1)

        taken = [together * i + k for k in range(together)]
        for r in range(16):
            for j in range(4):
                c = cb[j, r]
                for k, g in enumerate(taken):
                    pa[k, j, r + 8] = mbuf[j, pl.ds(r * mf + 8 * g, 8), :] * c
        filled = (0, 15)
        for step in range(1, SPREAD_PASSES + 1):
            src, dst = (pa, pb) if step % 2 else (pb, pa)

            def line(k, r):
                if not filled[0] <= r <= filled[1]:
                    return None
                return [src[k, j, r + 8] for j in range(4)]

            low = first_row(step)
            high = 15 - low
            above = [line(k, low - 1) for k in range(together)]
            here = [line(k, low) for k in range(together)]
            for r in range(low, high + 1):
                below = [line(k, r + 1) for k in range(together)]
                rate_r = [kb[j, r + 8] for j in range(4)]
                stay_r = [ab[j, r + 8] for j in range(4)] if here[0] is not None else None
                for k, g in enumerate(taken):
                    sides = beside(here[k], lane8) if stay_r is not None else None
                    for j in range(4):
                        parts = [row[k][j] for row in (above, below) if row[k] is not None]
                        if sides is not None:
                            parts.append(sides[j])
                        new = rate_r[j] * functools.reduce(lambda a, b: a + b, parts)
                        if stay_r is not None:
                            new = stay_r[j] * here[k][j] + new
                        if step < SPREAD_PASSES:
                            dst[k, j, r + 8] = new
                        elif r < 0:
                            halo_v[g, j, r + 4] = new
                        elif r >= 16:
                            halo_v[g, j, r - 12] = new
                        else:
                            acc[j, r + 4] += new * mbuf[j, pl.ds(r * mf + 8 * g, 8), :]
                above, here = here, below
            filled = (low, high)
        return carry

    lax.fori_loop(0, steps // together, spread_own, 0)

    wait_all(edge_coarse)
    rows = jnp.concatenate(
        [
            jnp.concatenate([coarse_e[side, q] for q in range(4)], axis=1)
            for side in range(2)
        ],
        axis=0,
    )
    out = split_dot(rows, perm[...])
    for j in range(4):
        cperm[j, 0:32] = out[:, 128 * j : 128 * j + 128]
    for side in range(2):
        known = (t > 0) if side == 0 else (t < tiles - 1)
        for j in range(4):
            for r in range(4):
                four = jnp.where(known, cperm[j, pl.ds(16 * side + r, 4, stride=4), :], 0.0)
                ceb[side, j, r, 0:4] = four
                ceb[side, j, r, 4:8] = four
    def spread_edge(side):
        wait_all(edge_members[side])
        only(down_end & feeder if side == 0 else up_end & feeder, onward[0][0].wait_recv)
        only(down_end & feeder if side == 0 else up_end & feeder, onward[1][0].wait_recv)

        def advance(old, step):
            base = 8 + (step - REACH if side == 0 else 16 - step)
            shift = 1 if side == 0 else -1
            nxt = []
            for i in range(4):
                terms = [old[i + shift + d] for d in (-1, 1) if 0 <= i + shift + d < 4]
                row = []
                same = old[i + shift] if 0 <= i + shift < 4 else None
                sides = beside(same, lane8) if same is not None else None
                for j in range(4):
                    parts = [term[j] for term in terms]
                    if sides is not None:
                        parts.append(sides[j])
                    around = functools.reduce(lambda a, b: a + b, parts)
                    new = kb[j, base + i] * around
                    if same is not None:
                        new = ab[j, base + i] * same[j] + new
                    row.append(new)
                nxt.append(row)
            return nxt

        def some(i, carry):
            groups_ = [together * i + k for k in range(together)]
            fields = []
            for r in range(4):
                for j in range(4):
                    to = r if side == 0 else 20 + r
                    total = acc[j, to]
                    for k, g in enumerate(groups_):
                        theirs = edge[side, j, pl.ds(r * mf + 8 * g, 8), :]
                        total = total + theirs * halo_v[g, j, 4 * side + r]
                        fields.append(theirs * ceb[side, j, r])
                    acc[j, to] = total
            olds = [
                [[fields[(4 * r + j) * together + k] for j in range(4)] for r in range(4)]
                for k in range(together)
            ]
            for step in range(1, SPREAD_PASSES + 1):
                olds = [advance(old, step) for old in olds]
            for i in range(4):
                r = i + (4 if side == 0 else 8)
                for j in range(4):
                    total = acc[j, r + 4]
                    for old, g in zip(olds, groups_):
                        total = total + old[i][j] * mbuf[j, pl.ds(r * mf + 8 * g, 8), :]
                    acc[j, r + 4] = total
            return carry

        lax.fori_loop(0, steps // together, some, 0)

    shares = [
        [
            send(
                part.at[lax.rem(m + o, groups), 48 * side : 48 * side + 48],
                got.at[o - 1, 48 * side : 48 * side + 48],
                o, 0, start=False,
            )
            for o in (1, 2, 3)
        ]
        for side in range(2)
    ]
    sub = lax.broadcasted_iota(jnp.int32, (6, 8, 128), 1)

    def share(side):
        folded = []
        for j in range(4):
            x = acc[j, 12 * side : 12 * side + 12]
            y = (x + pltpu.roll(x, 4, 1)).reshape(6, 2, 8, 128)
            folded.append(jnp.where(sub < 4, y[:, 0], y[:, 1]).reshape(48, 128))
        out = split_dot(jnp.concatenate(folded, axis=1), perm[...], transposed=True)
        for q in range(4):
            part[q, 48 * side : 48 * side + 48] = out[:, 128 * q : 128 * q + 128]
        for copy, _, _ in shares[side]:
            copy.start()

    def finish(side):
        only(there(0, 1 if side else -1), functools.partial(spread_edge, side))
        share(side)

    pl.when(~down_end)(functools.partial(finish, 0))
    finish(1)
    pl.when(down_end)(functools.partial(finish, 0))

    wait_all(rim_table)
    near = lax.broadcasted_iota(jnp.int32, (16, 128), 1) < 64
    side_on = jnp.where(near, (m < groups - 1).astype(jnp.int32), (m > 0).astype(jnp.int32)) > 0
    for a in range(4):
        both = jnp.where(near, table_col_in[1, a], table_col_in[0, a])
        table_h[a, 8:24] = jnp.where(side_on, both, 0.0)
    near1 = near[0:1]
    for side, first in ((0, 12), (1, 0)):
        on = (t > 0) if side == 0 else (t < tiles - 1)
        row = 7 if side == 0 else 24
        for b in range(4):
            table[first + b, row : row + 1] = jnp.where(on, table_row_in[side, 1, b : b + 1], 0.0)
        both = jnp.where(near1, table_row_in[side, 2, 0:1], table_row_in[side, 0, 3:4])
        table_h[first // 4, row : row + 1] = jnp.where(side_on[0:1] & on, both, 0.0)

    fetch_rate.wait()
    wait_all(rim_scale)
    unpack(scale_in, scale)
    for f in range(FIELDS):
        p = jnp.where(inside, rimmed(scale, f) * rimmed(grad, f), 0.0)
        for _ in range(STATIC_PASSES):
            around = (pltpu.roll(p, 1, 0) + pltpu.roll(p, 47, 0)) + (
                pltpu.roll(p, 1, 1) + pltpu.roll(p, 383, 1)
            )
            p = jnp.where(inside, p + rate_ref[f] * (around - 4.0 * p), 0.0)
        static_ref[f] = scale[f, 8:40, 128:384] * p[8:40, 0:256]

    wait_all(shares[0] + shares[1])
    esum[1] = (part[m] + got[0]) + (got[1] + got[2])
    rims = []
    for dm, dt in AROUND:
        slot = 1 - dm
        if dt == 0:
            rims.append(send_near(esum.at[1], esum.at[slot], dm, dt))
        elif dt == 1:
            rims.append(send_near(esum.at[1, 72:96], eup.at[slot], dm, dt))
        else:
            rims.append(send_near(esum.at[1, 0:24], edown.at[slot], dm, dt))
    wait_all(rims)
    members_all = member_count * groups

    def whole(slot):
        eall[slot] = esum[slot]
        eall[slot, 8:32] += eup[slot]
        eall[slot, 64:88] += edown[slot]

    for slot in range(3):
        whole(slot)
    lane96 = lax.broadcasted_iota(jnp.int32, (96, 128), 1)
    side_e = jnp.where(lane96 < 64, eall[2], eall[0]) / (members_all - 1)
    eall[1] = eall[1] / (members_all - 1)
    eall[0] = side_e
    for parity in range(2):
        pairs = [(1, 0), (3, -1)] if parity == 0 else [(2, 0), (0, 1)]
        for f in range(FIELDS):
            at_row = 16 * (4 * parity + f)
            mids = [eall[1, pl.ds(4 * (4 + d) + f, 16, stride=4), :] for _, d in pairs]
            ends = [eall[0, pl.ds(4 * (4 + d) + f, 16, stride=4), :] for _, d in pairs]
            for b in range(4):
                lhs[at_row : at_row + 16, 128 * b : 128 * b + 128] = (
                    table[4 * pairs[0][0] + b, 8:24] * mids[0]
                    + table[4 * pairs[1][0] + b, 8 + pairs[1][1] : 24 + pairs[1][1]] * mids[1]
                )
            lhs[at_row : at_row + 16, 512:640] = (
                table_h[pairs[0][0], 8:24] * ends[0]
                + table_h[pairs[1][0], 8 + pairs[1][1] : 24 + pairs[1][1]] * ends[1]
            )
    out = split_dot(lhs[...], place[...])
    for parity in range(2):
        for f in range(FIELDS):
            at_row = 16 * (4 * parity + f)
            for x in range(2):
                fine[x, pl.ds(32 * f + parity, 16, stride=2), :] = out[
                    at_row : at_row + 16, 128 * x : 128 * x + 128
                ]
    for f in range(FIELDS):
        for x in range(2):
            cols = slice(128 * x, 128 * x + 128)
            fine_ref[f, :, cols] = fine[x, 32 * f : 32 * f + 32]
    for copy, going, _ in sent:
        only(going, copy.wait_send)


def local(gradient, static_scale, static_rate, interp_index, interp_weight, members, spread_rate):
    member_count = members.shape[0]
    mf = member_count * FIELDS
    anywhere = pl.BlockSpec(memory_space=pl.ANY)
    vmem = pltpu.VMEM
    sems = 64
    static, fine = pl.pallas_call(
        kernel,
        out_shape=[jax.ShapeDtypeStruct(gradient.shape, F32)] * 2,
        in_specs=[anywhere] * 7,
        out_specs=[pl.BlockSpec(memory_space=pltpu.VMEM)] * 2,
        scratch_shapes=[
            vmem((4, 48, 512), F32),
            vmem((4, 48, 512), F32),
            vmem((2, 16, 256), F32),
            vmem((2, 16, 512), F32),
            vmem((2, 16, 256), F32),
            vmem((2, 16, 512), F32),
            vmem((4, 16, 128), jnp.int32),
            vmem((4, 16, 128), F32),
            vmem((2, 4, 16, 128), F32),
            vmem((2, 4, 16, 128), F32),
            vmem((2, 8, 128), F32),
            vmem((2, 3, 8, 128), F32),
            vmem((32, 512), F32),
            vmem(members.shape, BF16),
            vmem((512, 512), BF16),
            vmem((384, 512), BF16),
            vmem((640, 256), BF16),
            vmem((4, 16 * mf, 128), F32),
            vmem((2, 4, 4 * mf, 128), F32),
            vmem((2, 4, mf, 128), F32),
            vmem((16, 32, 128), F32),
            vmem((4, 32, 128), F32),
            vmem((4, 192, 128), F32),
            vmem((4, 4, 16, 128), F32),
            vmem((2, 4, 16, 128), F32),
            vmem((2, 4, 16, 128), F32),
            vmem((4, 64, 128), F32),
            vmem((4, 16, 8, 128), F32),
            vmem((2, 4, 4, 8, 128), F32),
            vmem((4, 32, 8, 128), F32),
            vmem((4, 32, 8, 128), F32),
            vmem((2, 4, 32, 8, 128), F32),
            vmem((2, 4, 32, 8, 128), F32),
            vmem((4, 24, 8, 128), F32),
            vmem((mf // 8, 4, 8, 8, 128), F32),
            vmem((4, 96, 128), F32),
            vmem((3, 96, 128), F32),
            vmem((3, 96, 128), F32),
            vmem((3, 24, 128), F32),
            vmem((3, 24, 128), F32),
            vmem((3, 96, 128), F32),
            vmem((128, 640), F32),
            vmem((2, 128, 128), F32),
            pltpu.SMEM((4,), F32),
            pltpu.SemaphoreType.DMA((7,)),
            pltpu.SemaphoreType.DMA((sems,)),
            pltpu.SemaphoreType.DMA((sems,)),
        ],
        compiler_params=pltpu.CompilerParams(
            collective_id=0, has_side_effects=True, vmem_limit_bytes=18 << 20
        ),
    )(*[pltpu.with_memory_space_constraint(x, pltpu.HBM) for x in (static_rate, gradient, static_scale, interp_index, interp_weight, members, spread_rate)])
    return 0.3 * static + 2.8 * fine


def solution(mesh):
    return jax.shard_map(
        local,
        mesh=mesh,
        in_specs=(
            P(None, "tile", "mem"),
            P(None, "tile", "mem"),
            P(),
            P(None, "tile", "mem"),
            P(None, "tile", "mem"),
            P("mem", None, "tile", None),
            P("tile", None),
        ),
        out_specs=P(None, "tile", "mem"),
        check_vma=False,
    )
```

```python
import functools

import jax
import jax.numpy as jnp
from jax import lax
from jax.experimental import pallas as pl
from jax.experimental.pallas import tpu as pltpu
from jax.sharding import PartitionSpec as P

STATIC_PASSES = 4
SPREAD_PASSES = 8
REACH = SPREAD_PASSES // 2
FIELDS = 4
MESH = pl.DeviceIdType.MESH
F32 = jnp.float32
BF16 = jnp.bfloat16
AROUND = [(0, 1), (0, -1), (1, 0), (-1, 0), (1, 1), (1, -1), (-1, 1), (-1, -1)]
ZROW = 16


def split_dot(x, one_hot, transposed=False):
    high = x.astype(BF16)
    rest = x - high.astype(F32)
    mid = rest.astype(BF16)
    low = (rest - mid.astype(F32)).astype(BF16)
    terms = jnp.concatenate([high, mid, low], axis=0)
    dims = (((1,), (1 if transposed else 0,)), ((), ()))
    out = lax.dot_general(terms, one_hot, dims, preferred_element_type=F32)
    n = x.shape[0]
    return (out[2 * n :] + out[n : 2 * n]) + out[:n]


def first_row(step):
    return max(-step, step - SPREAD_PASSES - REACH)


def beside(row, lane):
    axis = row[0].ndim - 1
    zero = jnp.zeros_like(row[0])
    left = jnp.where(lane == 0, zero, pltpu.roll(row[3], 1, axis))
    right = jnp.where(lane == 127, zero, pltpu.roll(row[0], 127, axis))
    return [left + row[1], row[0] + row[2], row[1] + row[3], row[2] + right]


def kernel(
    rate_hbm, grad_hbm, scale_hbm, index_hbm, weight_hbm, members_hbm, spread_hbm, static_ref, fine_ref,
    grad, scale, grad_out, grad_in, scale_out, scale_in, index, weight,
    table_col, table_col_in, table_row, table_row_in, spread, raw, perm, pick, place,
    mbuf, edge, passing, table, table_h, picked, coarse, coarse_out, coarse_e, cperm, cb, ceb, kb, ab,
    pa, pb, acc, halo_v, part, part_x, got, got_x, esum, eup, edown, eall, lhs, fine,
    rate_ref, local_sem, send_sem, recv_sem,
):
    m, t = lax.axis_index("mem"), lax.axis_index("tile")
    groups, tiles = lax.axis_size("mem"), lax.axis_size("tile")
    member_count = raw.shape[0]
    mf = member_count * FIELDS
    steps = mf // 8

    def at(dm, dt):
        return (lax.rem(m + dm + groups, groups), lax.rem(t + dt + tiles, tiles))

    def there(dm, dt):
        tests = []
        if dm:
            tests.append(m < groups - 1 if dm > 0 else m > 0)
        if dt:
            tests.append(t < tiles - 1 if dt > 0 else t > 0)
        return functools.reduce(jnp.logical_and, tests) if tests else None

    def only(test, action):
        if test is None:
            action()
        else:
            pl.when(test)(action)

    barrier = pltpu.get_barrier_semaphore()

    def greet(dm, dt):
        pl.semaphore_signal(barrier, inc=1, device_id=at(dm, dt), device_id_type=MESH)

    waited = 3
    for o in (1, 2, 3):
        greet(o, 0)
    for dm, dt in AROUND:
        if dt:
            only(there(dm, dt), functools.partial(greet, dm, dt))
            waited = waited + there(dm, dt).astype(jnp.int32)
    up_end, down_end = lax.rem(t, ZROW) == ZROW - 1, lax.rem(t, ZROW) == 0
    feeder = (up_end & (t < tiles - 1)) | (down_end & (t > 0))
    relay = (up_end | down_end) & ~feeder
    over = jnp.where(t < ZROW, ZROW, -ZROW)
    along = jnp.where(up_end, 1 - ZROW, ZROW - 1)

    @pl.when(up_end | down_end)
    def _():
        greet(0, over)
        greet(0, along)

    waited = waited + 2 * (up_end | down_end).astype(jnp.int32)

    locals_ = []

    def fetch(src, dst):
        copy = pltpu.make_async_copy(src, dst, local_sem.at[len(locals_)])
        locals_.append(copy)
        copy.start()
        return copy

    fetch_grad = fetch(grad_hbm, grad.at[:, 8:40, 128:384])
    fetch_members = fetch(members_hbm, raw)
    fetch_index = fetch(index_hbm, index)
    fetch_weight = fetch(weight_hbm, weight)
    fetch_spread = fetch(spread_hbm, spread.at[8:24])
    fetch_rate = fetch(rate_hbm, rate_ref)
    fetch_scale = fetch(scale_hbm, scale.at[:, 8:40, 128:384])

    sent = []

    def send(src, dst, dm, dt, going=None, coming=None, start=True):
        number = len(sent)
        copy = pltpu.make_async_remote_copy(
            src_ref=src, dst_ref=dst, send_sem=send_sem.at[number], recv_sem=recv_sem.at[number],
            device_id=at(dm, dt), device_id_type=MESH,
        )
        entry = (copy, going, coming)
        sent.append(entry)
        if start:
            only(entry[1], copy.start)
        return entry

    def send_near(src, dst, dm, dt):
        return send(src, dst, dm, dt, there(dm, dt), there(-dm, -dt))

    def pack(buf, out):
        for f in range(FIELDS):
            out[0, 4 * f : 4 * f + 4] = buf[f, 8:12, 128:384]
            out[1, 4 * f : 4 * f + 4] = buf[f, 36:40, 128:384]

    def send_rim(buf, out, come):
        copies = []
        for dm, dt in AROUND:
            col = {0: (128, 128, 256), 1: (256, 0, 128), -1: (128, 384, 128)}[dm]
            here, land = pl.ds(col[0], col[2]), pl.ds(col[1], col[2])
            if dt == 0:
                src, dst = buf.at[:, 8:40, here], buf.at[:, 8:40, land]
            else:
                side = 1 if dt > 0 else 0
                src = out.at[side, :, pl.ds(col[0] - 128, col[2])]
                dst = come.at[1 - side, :, land]
            copies.append(send_near(src, dst, dm, dt))
        return copies

    def unpack(come, buf):
        for f in range(FIELDS):
            buf[f, 4:8] = come[0, 4 * f : 4 * f + 4]
            buf[f, 40:44] = come[1, 4 * f : 4 * f + 4]

    def wait_all(copies):
        for copy, _, coming in copies:
            only(coming, copy.wait_recv)

    source = lax.broadcasted_iota(jnp.int32, (512, 512), 0)
    target = lax.broadcasted_iota(jnp.int32, (512, 512), 1)
    perm[...] = (source == 4 * (target & 127) + (target >> 7)).astype(F32).astype(BF16)

    fetch_members.wait()

    half = member_count // 2

    def convert(i):
        block = raw[half * i : half * i + half].reshape(half * FIELDS * 16, 512)
        for j in range(0, 4, 2):
            out = jnp.dot(
                block, perm[:, 128 * j : 128 * j + 256], preferred_element_type=F32
            )
            for q in range(half * FIELDS):
                for k in range(2):
                    mbuf[j + k, pl.ds(half * FIELDS * i + q, 16, stride=mf), :] = out[
                        16 * q : 16 * q + 16, 128 * k : 128 * k + 128
                    ]

    convert(0)
    convert(1)
    fetch_grad.wait()
    pack(grad, grad_out)
    fetch_spread.wait()
    pl.semaphore_wait(barrier, waited)
    rim_grad = send_rim(grad, grad_out, grad_in)
    rim_spread = [
        send_near(spread.at[16:24], spread.at[0:8], 0, 1),
        send_near(spread.at[8:16], spread.at[24:32], 0, -1),
    ]

    edge_members, late = [[], []], []
    for rows in (range(0, 1), range(1, 2), range(2, 4)):
        first, count = rows[0] * mf, len(rows) * mf
        for side, dt, cross, crossed in ((0, 1, up_end, down_end), (1, -1, down_end, up_end)):
            here = pl.ds(first + (12 * mf if side == 0 else 0), count)
            going, coming = there(0, dt), there(0, -dt)
            if rows[0] < 2:
                going, coming = going & ~cross, coming & ~crossed
            entry = send(
                mbuf.at[:, here], edge.at[side, :, pl.ds(first, count)], 0, dt, going, coming,
                start=False,
            )
            edge_members[side].append(entry)
            only(going & ~cross, entry[0].start)
            if rows[0] == 2:
                late.append((going & cross, entry[0]))
    origin = jnp.where(up_end, 12 * mf, 0)
    over_z, onward = [], []
    middle = mf + mf // 16 * 8
    for low, high in ((0, mf), (mf, middle), (middle, 2 * mf)):
        from_row = pl.ds(pl.multiple_of(origin + low, 8), high - low)
        rows = pl.ds(low, high - low)
        over_z.append(
            send(mbuf.at[:, from_row], passing.at[:, rows], 0, over, feeder, relay, start=low == 0)
        )
        onward.append(
            send(
                passing.at[:, rows], edge.at[down_end.astype(jnp.int32), :, rows],
                0, along, relay, feeder, start=False,
            )
        )
    late += [(feeder, copy) for copy, _, _ in over_z[1:]]

    fetch_index.wait()
    fetch_weight.wait()
    for o in range(16):
        total = jnp.zeros((16, 128), F32)
        for s in range(4):
            total = total + jnp.where(index[s] == o, weight[s], 0.0)
        table[o, 8:24] = total
        if o % 4 in (0, 3):
            table_col[o % 4 // 3, o // 4] = total
        if o < 4:
            table_row[0, o : o + 1] = total[0:1]
        if o >= 12:
            table_row[1, o - 12 : o - 11] = total[15:16]
    fetch_scale.wait()
    pack(scale, scale_out)
    source = lax.broadcasted_iota(jnp.int32, (384, 512), 0)
    target = lax.broadcasted_iota(jnp.int32, (384, 512), 1)
    wanted = 2 * (target & 127) + (target >> 7) - 1
    wanted = jnp.where(wanted < 0, 383, wanted)
    pick[...] = (source == wanted).astype(F32).astype(BF16)
    source = lax.broadcasted_iota(jnp.int32, (640, 256), 0)
    target = lax.broadcasted_iota(jnp.int32, (640, 256), 1)
    inner = (source < 512) & (target == 2 * (source & 127) + (source >> 7) - 1)
    left = (source == 639) & (target == 0)
    right = (source == 512) & (target == 255)
    place[...] = (inner | left | right).astype(F32).astype(BF16)

    rows48 = lax.broadcasted_iota(jnp.int32, (48, 384), 0)
    lanes48 = lax.broadcasted_iota(jnp.int32, (48, 384), 1)
    inside = (t > 0) | (rows48 >= 8)
    inside = inside & ((t < tiles - 1) | (rows48 < 40))
    inside = inside & ((m > 0) | (lanes48 < 320))
    inside = inside & ((m < groups - 1) | (lanes48 < 256) | (lanes48 >= 320))
    lane48 = lax.broadcasted_iota(jnp.int32, (48, 128), 1)

    def rimmed(buf, f):
        rim = jnp.where(lane48 < 64, buf[f, :, 384:512], buf[f, :, 0:128])
        return jnp.concatenate([buf[f, :, 128:384], rim], axis=1)

    wait_all(rim_grad)
    unpack(grad_in, grad)
    padded = jnp.concatenate(
        [jnp.where(inside, rimmed(grad, f), 0.0) for f in range(FIELDS)], axis=0
    )
    out = split_dot(padded, pick[...])
    for b in range(4):
        picked[b] = out[:, 128 * b : 128 * b + 128]
    for f in range(FIELDS):
        total = jnp.zeros((16, 128), F32)
        for a in range(4):
            for b in range(4):
                total = total + table[4 * a + b, 8:24] * picked[
                    b, pl.ds(48 * f + 7 + a, 16, stride=2), :
                ]
        coarse[m, f] = total
    all_coarse = [send(coarse.at[m], coarse.at[m], o, 0) for o in (1, 2, 3)]
    for test, copy in late:
        only(test, copy.start)

    wait_all(rim_spread)
    out = split_dot(spread[...], perm[...])
    row32 = lax.broadcasted_iota(jnp.int32, (32, 512), 0)
    known = ((t > 0) | (row32 >= 8)) & ((t < tiles - 1) | (row32 < 24))
    rate = jnp.where(known, out, 0.0)
    stay = jnp.where(known, 1.0 - 4.0 * out, 0.0)
    for j in range(4):
        for r in range(1, 31):
            kb[j, r] = jnp.broadcast_to(rate[r : r + 1, 128 * j : 128 * j + 128], (8, 128))
            ab[j, r] = jnp.broadcast_to(stay[r : r + 1, 128 * j : 128 * j + 128], (8, 128))
    acc[...] = jnp.zeros_like(acc)

    for side, dt in ((0, -1), (1, 1)):
        @pl.when(jnp.logical_not(there(0, dt)))
        def _():
            edge[side] = jnp.zeros_like(edge[side])

    for slot in range(3):
        for dt in (-1, 0, 1):
            if slot == 1 and dt == 0:
                continue
            dst = {-1: eup, 0: esum, 1: edown}[dt]

            @pl.when(jnp.logical_not(there(slot - 1, dt)))
            def _():
                dst[slot] = jnp.zeros_like(dst[slot])

    def pass_on(row):
        @pl.when(relay)
        def _():
            over_z[row][0].wait_recv()
            onward[row][0].start()

    wait_all(all_coarse)
    pass_on(0)
    for q in range(4):
        for f in range(FIELDS):
            coarse_out[0, q, 4 * f : 4 * f + 4] = coarse[q, f, 0:4]
            coarse_out[1, q, 4 * f : 4 * f + 4] = coarse[q, f, 12:16]
    edge_coarse = [
        send_near(coarse_out.at[1], coarse_e.at[0], 0, 1),
        send_near(coarse_out.at[0], coarse_e.at[1], 0, -1),
    ]
    rim_scale = send_rim(scale, scale_out, scale_in)
    rim_table = []
    for dm, dt in AROUND:
        if dt == 0:
            side = 1 if dm > 0 else 0
            rim_table.append(send_near(table_col.at[side], table_col_in.at[1 - side], dm, dt))
        else:
            side = 1 if dt > 0 else 0
            rim_table.append(
                send_near(table_row.at[side], table_row_in.at[1 - side, 1 - dm], dm, dt)
            )

    rows = jnp.concatenate([coarse[q].reshape(64, 128) for q in range(4)], axis=1)
    out = split_dot(rows, perm[...])
    for j in range(4):
        cperm[j, 0:64] = out[:, 128 * j : 128 * j + 128]
    for j in range(4):
        for r in range(16):
            four = cperm[j, pl.ds(r, 4, stride=16), :]
            cb[j, r, 0:4] = four
            cb[j, r, 4:8] = four

    lane8 = lax.broadcasted_iota(jnp.int32, (8, 128), 1)
    together = 2 if steps % 2 == 0 else 1

    def spread_own(i, carry):
        for piece, when in ((1, 1), (2, 3)):
            @pl.when(i == min(when, steps // together - 1))
            def _():
                pass_on(piece)

        taken = [together * i + k for k in range(together)]
        for r in range(16):
            for j in range(4):
                c = cb[j, r]
                for k, g in enumerate(taken):
                    pa[k, j, r + 8] = mbuf[j, pl.ds(r * mf + 8 * g, 8), :] * c
        filled = (0, 15)
        for step in range(1, SPREAD_PASSES + 1):
            src, dst = (pa, pb) if step % 2 else (pb, pa)

            def line(k, r):
                if not filled[0] <= r <= filled[1]:
                    return None
                return [src[k, j, r + 8] for j in range(4)]

            low = first_row(step)
            high = 15 - low
            above = [line(k, low - 1) for k in range(together)]
            here = [line(k, low) for k in range(together)]
            for r in range(low, high + 1):
                below = [line(k, r + 1) for k in range(together)]
                rate_r = [kb[j, r + 8] for j in range(4)]
                stay_r = [ab[j, r + 8] for j in range(4)] if here[0] is not None else None
                for k, g in enumerate(taken):
                    sides = beside(here[k], lane8) if stay_r is not None else None
                    for j in range(4):
                        parts = [row[k][j] for row in (above, below) if row[k] is not None]
                        if sides is not None:
                            parts.append(sides[j])
                        new = rate_r[j] * functools.reduce(lambda a, b: a + b, parts)
                        if stay_r is not None:
                            new = stay_r[j] * here[k][j] + new
                        if step < SPREAD_PASSES:
                            dst[k, j, r + 8] = new
                        elif r < 0:
                            halo_v[g, j, r + 4] = new
                        elif r >= 16:
                            halo_v[g, j, r - 12] = new
                        else:
                            acc[j, r + 4] += new * mbuf[j, pl.ds(r * mf + 8 * g, 8), :]
                above, here = here, below
            filled = (low, high)
        return carry

    lax.fori_loop(0, steps // together, spread_own, 0)

    wait_all(edge_coarse)
    rows = jnp.concatenate(
        [
            jnp.concatenate([coarse_e[side, q] for q in range(4)], axis=1)
            for side in range(2)
        ],
        axis=0,
    )
    out = split_dot(rows, perm[...])
    for j in range(4):
        cperm[j, 0:32] = out[:, 128 * j : 128 * j + 128]
    for side in range(2):
        known = (t > 0) if side == 0 else (t < tiles - 1)
        for j in range(4):
            for r in range(4):
                four = jnp.where(known, cperm[j, pl.ds(16 * side + r, 4, stride=4), :], 0.0)
                ceb[side, j, r, 0:4] = four
                ceb[side, j, r, 4:8] = four
    def meet_edge(side):
        wait_all(edge_members[side])
        for copy, _, _ in onward:
            only(down_end & feeder if side == 0 else up_end & feeder, copy.wait_recv)

        for r in range(4):
            for j in range(4):
                terms = [
                    edge[side, j, pl.ds(r * mf + 8 * g, 8), :] * halo_v[g, j, 4 * side + r]
                    for g in range(steps)
                ]
                acc[j, r if side == 0 else 20 + r] = functools.reduce(lambda a, b: a + b, terms)

    def spread_edge(side):
        def advance(old, step):
            base = 8 + (step - REACH if side == 0 else 16 - step)
            shift = 1 if side == 0 else -1
            nxt = []
            for i in range(4):
                terms = [old[i + shift + d] for d in (-1, 1) if 0 <= i + shift + d < 4]
                row = []
                same = old[i + shift] if 0 <= i + shift < 4 else None
                sides = beside(same, lane8) if same is not None else None
                for j in range(4):
                    parts = [term[j] for term in terms]
                    if sides is not None:
                        parts.append(sides[j])
                    around = functools.reduce(lambda a, b: a + b, parts)
                    new = kb[j, base + i] * around
                    if same is not None:
                        new = ab[j, base + i] * same[j] + new
                    row.append(new)
                nxt.append(row)
            return nxt

        def some(i, carry):
            groups_ = [together * i + k for k in range(together)]
            fields = []
            for r in range(4):
                for j in range(4):
                    for g in groups_:
                        theirs = edge[side, j, pl.ds(r * mf + 8 * g, 8), :]
                        fields.append(theirs * ceb[side, j, r])
            olds = [
                [[fields[(4 * r + j) * together + k] for j in range(4)] for r in range(4)]
                for k in range(together)
            ]
            for step in range(1, SPREAD_PASSES + 1):
                olds = [advance(old, step) for old in olds]
            for i in range(4):
                r = i + (4 if side == 0 else 8)
                for j in range(4):
                    total = acc[j, r + 4]
                    for old, g in zip(olds, groups_):
                        total = total + old[i][j] * mbuf[j, pl.ds(r * mf + 8 * g, 8), :]
                    acc[j, r + 4] = total
            return carry

        lax.fori_loop(0, steps // together, some, 0)

    spans = [(0, 32), (64, 96), (32, 64)]
    shares = []
    for low, high in spans:
        shares.append(
            [
                send(
                    part.at[lax.rem(m + o, groups), low:high], got.at[o - 1, low:high], o, 0,
                    start=False,
                )
                for o in (1, 2, 3)
            ]
        )
    shares[2] += [
        send(part_x.at[lax.rem(m + o, groups)], got_x.at[o - 1], o, 0, start=False)
        for o in (1, 2, 3)
    ]
    sub = lax.broadcasted_iota(jnp.int32, (4, 8, 128), 1)
    near32 = lax.broadcasted_iota(jnp.int32, (32, 128), 1) < 64

    def share(piece):
        low, high = spans[piece]
        folded = []
        for j in range(4):
            x = acc[j, low // 4 : high // 4]
            y = (x + pltpu.roll(x, 4, 1)).reshape(4, 2, 8, 128)
            folded.append(jnp.where(sub < 4, y[:, 0], y[:, 1]).reshape(32, 128))
        out = split_dot(jnp.concatenate(folded, axis=1), perm[...], transposed=True)
        quarters = [out[:, 128 * q : 128 * q + 128] for q in range(4)]
        for q in range(4):
            part[q, low:high] = quarters[q]
            if piece == 2:
                part_x[q] = jnp.where(near32, quarters[min(q + 1, 3)], quarters[max(q - 1, 0)])
        for copy, _, _ in shares[piece]:
            copy.start()

    def finish(side):
        exists = there(0, 1 if side else -1)
        only(exists, functools.partial(meet_edge, side))
        share(side)
        only(exists, functools.partial(spread_edge, side))

    pl.when(~down_end)(functools.partial(finish, 0))
    finish(1)
    pl.when(down_end)(functools.partial(finish, 0))
    share(2)

    wait_all(rim_table)
    near = lax.broadcasted_iota(jnp.int32, (16, 128), 1) < 64
    side_on = jnp.where(near, (m < groups - 1).astype(jnp.int32), (m > 0).astype(jnp.int32)) > 0
    for a in range(4):
        both = jnp.where(near, table_col_in[1, a], table_col_in[0, a])
        table_h[a, 8:24] = jnp.where(side_on, both, 0.0)
    near1 = near[0:1]
    for side, first in ((0, 12), (1, 0)):
        on = (t > 0) if side == 0 else (t < tiles - 1)
        row = 7 if side == 0 else 24
        for b in range(4):
            table[first + b, row : row + 1] = jnp.where(on, table_row_in[side, 1, b : b + 1], 0.0)
        both = jnp.where(near1, table_row_in[side, 2, 0:1], table_row_in[side, 0, 3:4])
        table_h[first // 4, row : row + 1] = jnp.where(side_on[0:1] & on, both, 0.0)

    rims = []
    for piece, (low, high) in enumerate(spans[:2]):
        wait_all(shares[piece])
        esum[1, low:high] = (part[m, low:high] + got[0, low:high]) + (
            got[1, low:high] + got[2, low:high]
        )
    for dm, dt in AROUND:
        slot = 1 - dm
        if dt == 0:
            for low, high in spans[:2]:
                rims.append(send_near(esum.at[1, low:high], esum.at[slot, low:high], dm, dt))
        elif dt == 1:
            rims.append(send_near(esum.at[1, 72:96], eup.at[slot], dm, dt))
        else:
            rims.append(send_near(esum.at[1, 0:24], edown.at[slot], dm, dt))

    fetch_rate.wait()
    wait_all(rim_scale)
    unpack(scale_in, scale)
    for f in range(FIELDS):
        p = jnp.where(inside, rimmed(scale, f) * rimmed(grad, f), 0.0)
        for _ in range(STATIC_PASSES):
            around = (pltpu.roll(p, 1, 0) + pltpu.roll(p, 47, 0)) + (
                pltpu.roll(p, 1, 1) + pltpu.roll(p, 383, 1)
            )
            p = jnp.where(inside, p + rate_ref[f] * (around - 4.0 * p), 0.0)
        static_ref[f] = scale[f, 8:40, 128:384] * p[8:40, 0:256]

    wait_all(shares[2])
    esum[1, 32:64] = (part[m, 32:64] + got[0, 32:64]) + (got[1, 32:64] + got[2, 32:64])
    wait_all(rims)
    members_all = member_count * groups

    def whole(slot):
        for low, high in spans if slot == 1 else spans[:2]:
            eall[slot, low:high] = esum[slot, low:high]
        eall[slot, 8:32] += eup[slot]
        eall[slot, 64:88] += edown[slot]

    for slot in range(3):
        whole(slot)
    lane96 = lax.broadcasted_iota(jnp.int32, (96, 128), 1)
    side_e = jnp.where(lane96 < 64, eall[2], eall[0]) / (members_all - 1)
    eall[1] = eall[1] / (members_all - 1)
    eall[0] = side_e
    eall[0, 32:64] = ((part_x[m] + got_x[0]) + (got_x[1] + got_x[2])) / (members_all - 1)
    for parity in range(2):
        pairs = [(1, 0), (3, -1)] if parity == 0 else [(2, 0), (0, 1)]
        for f in range(FIELDS):
            at_row = 16 * (4 * parity + f)
            mids = [eall[1, pl.ds(4 * (4 + d) + f, 16, stride=4), :] for _, d in pairs]
            ends = [eall[0, pl.ds(4 * (4 + d) + f, 16, stride=4), :] for _, d in pairs]
            for b in range(4):
                lhs[at_row : at_row + 16, 128 * b : 128 * b + 128] = (
                    table[4 * pairs[0][0] + b, 8:24] * mids[0]
                    + table[4 * pairs[1][0] + b, 8 + pairs[1][1] : 24 + pairs[1][1]] * mids[1]
                )
            lhs[at_row : at_row + 16, 512:640] = (
                table_h[pairs[0][0], 8:24] * ends[0]
                + table_h[pairs[1][0], 8 + pairs[1][1] : 24 + pairs[1][1]] * ends[1]
            )
    out = split_dot(lhs[...], place[...])
    for parity in range(2):
        for f in range(FIELDS):
            at_row = 16 * (4 * parity + f)
            for x in range(2):
                fine[x, pl.ds(32 * f + parity, 16, stride=2), :] = out[
                    at_row : at_row + 16, 128 * x : 128 * x + 128
                ]
    for f in range(FIELDS):
        for x in range(2):
            cols = slice(128 * x, 128 * x + 128)
            fine_ref[f, :, cols] = fine[x, 32 * f : 32 * f + 32]
    for copy, going, _ in sent:
        only(going, copy.wait_send)


def local(gradient, static_scale, static_rate, interp_index, interp_weight, members, spread_rate):
    member_count = members.shape[0]
    mf = member_count * FIELDS
    anywhere = pl.BlockSpec(memory_space=pl.ANY)
    vmem = pltpu.VMEM
    sems = 80
    static, fine = pl.pallas_call(
        kernel,
        out_shape=[jax.ShapeDtypeStruct(gradient.shape, F32)] * 2,
        in_specs=[anywhere] * 7,
        out_specs=[pl.BlockSpec(memory_space=pltpu.VMEM)] * 2,
        scratch_shapes=[
            vmem((4, 48, 512), F32),
            vmem((4, 48, 512), F32),
            vmem((2, 16, 256), F32),
            vmem((2, 16, 512), F32),
            vmem((2, 16, 256), F32),
            vmem((2, 16, 512), F32),
            vmem((4, 16, 128), jnp.int32),
            vmem((4, 16, 128), F32),
            vmem((2, 4, 16, 128), F32),
            vmem((2, 4, 16, 128), F32),
            vmem((2, 8, 128), F32),
            vmem((2, 3, 8, 128), F32),
            vmem((32, 512), F32),
            vmem(members.shape, BF16),
            vmem((512, 512), BF16),
            vmem((384, 512), BF16),
            vmem((640, 256), BF16),
            vmem((4, 16 * mf, 128), F32),
            vmem((2, 4, 4 * mf, 128), F32),
            vmem((4, 2 * mf, 128), F32),
            vmem((16, 32, 128), F32),
            vmem((4, 32, 128), F32),
            vmem((4, 192, 128), F32),
            vmem((4, 4, 16, 128), F32),
            vmem((2, 4, 16, 128), F32),
            vmem((2, 4, 16, 128), F32),
            vmem((4, 64, 128), F32),
            vmem((4, 16, 8, 128), F32),
            vmem((2, 4, 4, 8, 128), F32),
            vmem((4, 32, 8, 128), F32),
            vmem((4, 32, 8, 128), F32),
            vmem((2, 4, 32, 8, 128), F32),
            vmem((2, 4, 32, 8, 128), F32),
            vmem((4, 24, 8, 128), F32),
            vmem((mf // 8, 4, 8, 8, 128), F32),
            vmem((4, 96, 128), F32),
            vmem((4, 32, 128), F32),
            vmem((3, 96, 128), F32),
            vmem((3, 32, 128), F32),
            vmem((3, 96, 128), F32),
            vmem((3, 24, 128), F32),
            vmem((3, 24, 128), F32),
            vmem((3, 96, 128), F32),
            vmem((128, 640), F32),
            vmem((2, 128, 128), F32),
            pltpu.SMEM((4,), F32),
            pltpu.SemaphoreType.DMA((7,)),
            pltpu.SemaphoreType.DMA((sems,)),
            pltpu.SemaphoreType.DMA((sems,)),
        ],
        compiler_params=pltpu.CompilerParams(
            collective_id=0, has_side_effects=True, vmem_limit_bytes=18 << 20
        ),
    )(*[pltpu.with_memory_space_constraint(x, pltpu.HBM) for x in (static_rate, gradient, static_scale, interp_index, interp_weight, members, spread_rate)])
    return 0.3 * static + 2.8 * fine


def solution(mesh):
    return jax.shard_map(
        local,
        mesh=mesh,
        in_specs=(
            P(None, "tile", "mem"),
            P(None, "tile", "mem"),
            P(),
            P(None, "tile", "mem"),
            P(None, "tile", "mem"),
            P("mem", None, "tile", None),
            P("tile", None),
        ),
        out_specs=P(None, "tile", "mem"),
        check_vma=False,
    )
```

```python
import functools

import jax
import jax.numpy as jnp
from jax import lax
from jax.experimental import pallas as pl
from jax.experimental.pallas import tpu as pltpu
from jax.sharding import PartitionSpec as P

STATIC_PASSES = 4
SPREAD_PASSES = 8
REACH = SPREAD_PASSES // 2
FIELDS = 4
MESH = pl.DeviceIdType.MESH
F32 = jnp.float32
BF16 = jnp.bfloat16
AROUND = [(0, 1), (0, -1), (1, 0), (-1, 0), (1, 1), (1, -1), (-1, 1), (-1, -1)]
ZROW = 16


def split_dot(x, one_hot, transposed=False):
    high = x.astype(BF16)
    rest = x - high.astype(F32)
    mid = rest.astype(BF16)
    low = (rest - mid.astype(F32)).astype(BF16)
    terms = jnp.concatenate([high, mid, low], axis=0)
    dims = (((1,), (1 if transposed else 0,)), ((), ()))
    out = lax.dot_general(terms, one_hot, dims, preferred_element_type=F32)
    n = x.shape[0]
    return (out[2 * n :] + out[n : 2 * n]) + out[:n]


def first_row(step):
    return max(-step, step - SPREAD_PASSES - REACH)


def beside(row, lane):
    axis = row[0].ndim - 1
    zero = jnp.zeros_like(row[0])
    left = jnp.where(lane == 0, zero, pltpu.roll(row[3], 1, axis))
    right = jnp.where(lane == 127, zero, pltpu.roll(row[0], 127, axis))
    return [left + row[1], row[0] + row[2], row[1] + row[3], row[2] + right]


def kernel(
    rate_hbm, grad_hbm, scale_hbm, index_hbm, weight_hbm, members_hbm, spread_hbm, static_ref, fine_ref,
    grad, scale, grad_out, grad_in, scale_out, scale_in, index, weight,
    table_col, table_col_in, spread, raw, perm, pick, place,
    mbuf, edge, passing, table, table_h, picked, coarse, coarse_out, coarse_e, cperm, cb, ceb, kb, ab,
    pa, pb, acc, halo_v, part, part_x, got, got_x, esum, eup, edown, eall, lhs, fine,
    rate_ref, local_sem, send_sem, recv_sem,
):
    m, t = lax.axis_index("mem"), lax.axis_index("tile")
    groups, tiles = lax.axis_size("mem"), lax.axis_size("tile")
    member_count = raw.shape[0]
    mf = member_count * FIELDS
    steps = mf // 8

    def at(dm, dt):
        return (lax.rem(m + dm + groups, groups), lax.rem(t + dt + tiles, tiles))

    def there(dm, dt):
        tests = []
        if dm:
            tests.append(m < groups - 1 if dm > 0 else m > 0)
        if dt:
            tests.append(t < tiles - 1 if dt > 0 else t > 0)
        return functools.reduce(jnp.logical_and, tests) if tests else None

    def only(test, action):
        if test is None:
            action()
        else:
            pl.when(test)(action)

    barrier = pltpu.get_barrier_semaphore()

    def greet(dm, dt):
        pl.semaphore_signal(barrier, inc=1, device_id=at(dm, dt), device_id_type=MESH)

    waited = 3
    for o in (1, 2, 3):
        greet(o, 0)
    for dm, dt in AROUND:
        if dt:
            only(there(dm, dt), functools.partial(greet, dm, dt))
            waited = waited + there(dm, dt).astype(jnp.int32)
    up_end, down_end = lax.rem(t, ZROW) == ZROW - 1, lax.rem(t, ZROW) == 0
    feeder = (up_end & (t < tiles - 1)) | (down_end & (t > 0))
    relay = (up_end | down_end) & ~feeder
    over = jnp.where(t < ZROW, ZROW, -ZROW)
    along = jnp.where(up_end, 1 - ZROW, ZROW - 1)

    @pl.when(up_end | down_end)
    def _():
        greet(0, over)
        greet(0, along)

    waited = waited + 2 * (up_end | down_end).astype(jnp.int32)

    locals_ = []

    def fetch(src, dst):
        copy = pltpu.make_async_copy(src, dst, local_sem.at[len(locals_)])
        locals_.append(copy)
        copy.start()
        return copy

    fetch_grad = fetch(grad_hbm, grad.at[:, 8:40, 128:384])
    fetch_members = fetch(members_hbm, raw)
    fetch_index = fetch(index_hbm, index)
    fetch_weight = fetch(weight_hbm, weight)
    fetch_spread = fetch(spread_hbm, spread.at[8:24])
    fetch_rate = fetch(rate_hbm, rate_ref)
    fetch_scale = fetch(scale_hbm, scale.at[:, 8:40, 128:384])

    sent = []

    def send(src, dst, dm, dt, going=None, coming=None, start=True):
        number = len(sent)
        copy = pltpu.make_async_remote_copy(
            src_ref=src, dst_ref=dst, send_sem=send_sem.at[number], recv_sem=recv_sem.at[number],
            device_id=at(dm, dt), device_id_type=MESH,
        )
        entry = (copy, going, coming)
        sent.append(entry)
        if start:
            only(entry[1], copy.start)
        return entry

    def send_near(src, dst, dm, dt):
        return send(src, dst, dm, dt, there(dm, dt), there(-dm, -dt))

    def pack(buf, out):
        for f in range(FIELDS):
            out[0, 4 * f : 4 * f + 4] = buf[f, 8:12, 128:384]
            out[1, 4 * f : 4 * f + 4] = buf[f, 36:40, 128:384]

    def send_rim(buf, out, come):
        copies = []
        for dm, dt in AROUND:
            col = {0: (128, 128, 256), 1: (256, 0, 128), -1: (128, 384, 128)}[dm]
            here, land = pl.ds(col[0], col[2]), pl.ds(col[1], col[2])
            if dt == 0:
                src, dst = buf.at[:, 8:40, here], buf.at[:, 8:40, land]
            else:
                side = 1 if dt > 0 else 0
                src = out.at[side, :, pl.ds(col[0] - 128, col[2])]
                dst = come.at[1 - side, :, land]
            copies.append(send_near(src, dst, dm, dt))
        return copies

    def unpack(come, buf):
        for f in range(FIELDS):
            buf[f, 4:8] = come[0, 4 * f : 4 * f + 4]
            buf[f, 40:44] = come[1, 4 * f : 4 * f + 4]

    def wait_all(copies):
        for copy, _, coming in copies:
            only(coming, copy.wait_recv)

    source = lax.broadcasted_iota(jnp.int32, (512, 512), 0)
    target = lax.broadcasted_iota(jnp.int32, (512, 512), 1)
    perm[...] = (source == 4 * (target & 127) + (target >> 7)).astype(F32).astype(BF16)

    fetch_members.wait()

    half = member_count // 2

    def convert(i):
        block = raw[half * i : half * i + half].reshape(half * FIELDS * 16, 512)
        for j in range(0, 4, 2):
            out = jnp.dot(
                block, perm[:, 128 * j : 128 * j + 256], preferred_element_type=F32
            )
            for q in range(half * FIELDS):
                for k in range(2):
                    mbuf[j + k, pl.ds(half * FIELDS * i + q, 16, stride=mf), :] = out[
                        16 * q : 16 * q + 16, 128 * k : 128 * k + 128
                    ]

    convert(0)
    convert(1)
    fetch_grad.wait()
    pack(grad, grad_out)
    fetch_spread.wait()
    pl.semaphore_wait(barrier, waited)
    rim_grad = send_rim(grad, grad_out, grad_in)
    rim_spread = [
        send_near(spread.at[16:24], spread.at[0:8], 0, 1),
        send_near(spread.at[8:16], spread.at[24:32], 0, -1),
    ]

    edge_members, late = [[], []], []
    for rows in (range(0, 2), range(2, 4)):
        first, count = rows[0] * mf, len(rows) * mf
        for side, dt, cross, crossed in ((0, 1, up_end, down_end), (1, -1, down_end, up_end)):
            here = pl.ds(first + (12 * mf if side == 0 else 0), count)
            going, coming = there(0, dt), there(0, -dt)
            if rows[0] == 0:
                going, coming = going & ~cross, coming & ~crossed
            entry = send(
                mbuf.at[:, here], edge.at[side, :, pl.ds(first, count)], 0, dt, going, coming,
                start=False,
            )
            edge_members[side].append(entry)
            only(going & ~cross, entry[0].start)
            if rows[0] == 2:
                late.append((going & cross, entry[0]))
    origin = jnp.where(up_end, 12 * mf, 0)
    over_z, onward = [], []
    middle = mf + mf // 16 * 8
    for low, high in ((0, mf), (mf, middle), (middle, 2 * mf)):
        from_row = pl.ds(pl.multiple_of(origin + low, 8), high - low)
        rows = pl.ds(low, high - low)
        over_z.append(
            send(mbuf.at[:, from_row], passing.at[:, rows], 0, over, feeder, relay, start=low == 0)
        )
        onward.append(
            send(
                passing.at[:, rows], edge.at[down_end.astype(jnp.int32), :, rows],
                0, along, relay, feeder, start=False,
            )
        )
    late += [(feeder, copy) for copy, _, _ in over_z[1:]]

    fetch_index.wait()
    fetch_weight.wait()
    for o in range(16):
        total = jnp.zeros((16, 128), F32)
        for s in range(4):
            total = total + jnp.where(index[s] == o, weight[s], 0.0)
        table[o, 8:24] = total
        if o % 4 in (0, 3):
            table_col[o % 4 // 3, o // 4] = total
        for x in (0, 128):
            if o < 4:
                scale_out[0, 16 + o : 17 + o, x : x + 128] = total[0:1]
            if o >= 12:
                scale_out[1, 4 + o : 5 + o, x : x + 128] = total[15:16]
    fetch_scale.wait()
    pack(scale, scale_out)
    source = lax.broadcasted_iota(jnp.int32, (384, 512), 0)
    target = lax.broadcasted_iota(jnp.int32, (384, 512), 1)
    wanted = 2 * (target & 127) + (target >> 7) - 1
    wanted = jnp.where(wanted < 0, 383, wanted)
    pick[...] = (source == wanted).astype(F32).astype(BF16)
    source = lax.broadcasted_iota(jnp.int32, (640, 256), 0)
    target = lax.broadcasted_iota(jnp.int32, (640, 256), 1)
    inner = (source < 512) & (target == 2 * (source & 127) + (source >> 7) - 1)
    left = (source == 639) & (target == 0)
    right = (source == 512) & (target == 255)
    place[...] = (inner | left | right).astype(F32).astype(BF16)

    rows48 = lax.broadcasted_iota(jnp.int32, (48, 384), 0)
    lanes48 = lax.broadcasted_iota(jnp.int32, (48, 384), 1)
    inside = (t > 0) | (rows48 >= 8)
    inside = inside & ((t < tiles - 1) | (rows48 < 40))
    inside = inside & ((m > 0) | (lanes48 < 320))
    inside = inside & ((m < groups - 1) | (lanes48 < 256) | (lanes48 >= 320))
    lane48 = lax.broadcasted_iota(jnp.int32, (48, 128), 1)

    def rimmed(buf, f):
        rim = jnp.where(lane48 < 64, buf[f, :, 384:512], buf[f, :, 0:128])
        return jnp.concatenate([buf[f, :, 128:384], rim], axis=1)

    wait_all(rim_grad)
    unpack(grad_in, grad)
    padded = jnp.concatenate(
        [jnp.where(inside, rimmed(grad, f), 0.0) for f in range(FIELDS)], axis=0
    )
    out = split_dot(padded, pick[...])
    for b in range(4):
        picked[b] = out[:, 128 * b : 128 * b + 128]
    for f in range(FIELDS):
        total = jnp.zeros((16, 128), F32)
        for a in range(4):
            for b in range(4):
                total = total + table[4 * a + b, 8:24] * picked[
                    b, pl.ds(48 * f + 7 + a, 16, stride=2), :
                ]
        coarse[m, f] = total
    all_coarse = [send(coarse.at[m], coarse.at[m], o, 0) for o in (1, 2, 3)]
    for test, copy in late:
        only(test, copy.start)

    wait_all(rim_spread)
    out = split_dot(spread[...], perm[...])
    row32 = lax.broadcasted_iota(jnp.int32, (32, 512), 0)
    known = ((t > 0) | (row32 >= 8)) & ((t < tiles - 1) | (row32 < 24))
    rate = jnp.where(known, out, 0.0)
    stay = jnp.where(known, 1.0 - 4.0 * out, 0.0)
    for j in range(4):
        for r in range(1, 31):
            kb[j, r] = jnp.broadcast_to(rate[r : r + 1, 128 * j : 128 * j + 128], (8, 128))
            ab[j, r] = jnp.broadcast_to(stay[r : r + 1, 128 * j : 128 * j + 128], (8, 128))
    acc[...] = jnp.zeros_like(acc)

    for side, dt in ((0, -1), (1, 1)):
        @pl.when(jnp.logical_not(there(0, dt)))
        def _():
            edge[side] = jnp.zeros_like(edge[side])

    for slot in range(3):
        for dt in (-1, 0, 1):
            if slot == 1 and dt == 0:
                continue
            dst = {-1: eup, 0: esum, 1: edown}[dt]

            @pl.when(jnp.logical_not(there(slot - 1, dt)))
            def _():
                dst[slot] = jnp.zeros_like(dst[slot])

    def pass_on(row):
        @pl.when(relay)
        def _():
            over_z[row][0].wait_recv()
            onward[row][0].start()

    wait_all(all_coarse)
    pass_on(0)
    for q in range(4):
        for f in range(FIELDS):
            coarse_out[0, q, 4 * f : 4 * f + 4] = coarse[q, f, 0:4]
            coarse_out[1, q, 4 * f : 4 * f + 4] = coarse[q, f, 12:16]
    edge_coarse = [
        send_near(coarse_out.at[1], coarse_e.at[0], 0, 1),
        send_near(coarse_out.at[0], coarse_e.at[1], 0, -1),
    ]
    rim_scale = send_rim(scale, scale_out, scale_in)
    rim_table = []
    for dm, dt in AROUND:
        if dt == 0:
            side = 1 if dm > 0 else 0
            rim_table.append(send_near(table_col.at[side], table_col_in.at[1 - side], dm, dt))

    rows = jnp.concatenate([coarse[q].reshape(64, 128) for q in range(4)], axis=1)
    out = split_dot(rows, perm[...])
    for j in range(4):
        cperm[j, 0:64] = out[:, 128 * j : 128 * j + 128]
    for j in range(4):
        for r in range(16):
            four = cperm[j, pl.ds(r, 4, stride=16), :]
            cb[j, r, 0:4] = four
            cb[j, r, 4:8] = four

    lane8 = lax.broadcasted_iota(jnp.int32, (8, 128), 1)
    together = 2 if steps % 2 == 0 else 1

    def spread_own(i, carry):
        for piece, when in ((1, 1), (2, 3)):
            @pl.when(i == min(when, steps // together - 1))
            def _():
                pass_on(piece)

        taken = [together * i + k for k in range(together)]
        for r in range(16):
            for j in range(4):
                c = cb[j, r]
                for k, g in enumerate(taken):
                    pa[k, j, r + 8] = mbuf[j, pl.ds(r * mf + 8 * g, 8), :] * c
        filled = (0, 15)
        for step in range(1, SPREAD_PASSES + 1):
            src, dst = (pa, pb) if step % 2 else (pb, pa)

            def line(k, r):
                if not filled[0] <= r <= filled[1]:
                    return None
                return [src[k, j, r + 8] for j in range(4)]

            low = first_row(step)
            high = 15 - low
            above = [line(k, low - 1) for k in range(together)]
            here = [line(k, low) for k in range(together)]
            for r in range(low, high + 1):
                below = [line(k, r + 1) for k in range(together)]
                rate_r = [kb[j, r + 8] for j in range(4)]
                stay_r = [ab[j, r + 8] for j in range(4)] if here[0] is not None else None
                for k, g in enumerate(taken):
                    sides = beside(here[k], lane8) if stay_r is not None else None
                    for j in range(4):
                        parts = [row[k][j] for row in (above, below) if row[k] is not None]
                        if sides is not None:
                            parts.append(sides[j])
                        new = rate_r[j] * functools.reduce(lambda a, b: a + b, parts)
                        if stay_r is not None:
                            new = stay_r[j] * here[k][j] + new
                        if step < SPREAD_PASSES:
                            dst[k, j, r + 8] = new
                        elif r < 0:
                            halo_v[g, j, r + 4] = new
                        elif r >= 16:
                            halo_v[g, j, r - 12] = new
                        else:
                            acc[j, r + 4] += new * mbuf[j, pl.ds(r * mf + 8 * g, 8), :]
                above, here = here, below
            filled = (low, high)
        return carry

    lax.fori_loop(0, steps // together, spread_own, 0)

    wait_all(edge_coarse)
    rows = jnp.concatenate(
        [
            jnp.concatenate([coarse_e[side, q] for q in range(4)], axis=1)
            for side in range(2)
        ],
        axis=0,
    )
    out = split_dot(rows, perm[...])
    for j in range(4):
        cperm[j, 0:32] = out[:, 128 * j : 128 * j + 128]
    for side in range(2):
        known = (t > 0) if side == 0 else (t < tiles - 1)
        for j in range(4):
            for r in range(4):
                four = jnp.where(known, cperm[j, pl.ds(16 * side + r, 4, stride=4), :], 0.0)
                ceb[side, j, r, 0:4] = four
                ceb[side, j, r, 4:8] = four
    def meet_edge(side):
        wait_all(edge_members[side])
        for copy, _, _ in onward:
            only(down_end & feeder if side == 0 else up_end & feeder, copy.wait_recv)

        for r in range(4):
            for j in range(4):
                terms = [
                    edge[side, j, pl.ds(r * mf + 8 * g, 8), :] * halo_v[g, j, 4 * side + r]
                    for g in range(steps)
                ]
                acc[j, r if side == 0 else 20 + r] = functools.reduce(lambda a, b: a + b, terms)

    def spread_edge(side):
        def advance(old, step):
            base = 8 + (step - REACH if side == 0 else 16 - step)
            shift = 1 if side == 0 else -1
            nxt = []
            for i in range(4):
                terms = [old[i + shift + d] for d in (-1, 1) if 0 <= i + shift + d < 4]
                row = []
                same = old[i + shift] if 0 <= i + shift < 4 else None
                sides = beside(same, lane8) if same is not None else None
                for j in range(4):
                    parts = [term[j] for term in terms]
                    if sides is not None:
                        parts.append(sides[j])
                    around = functools.reduce(lambda a, b: a + b, parts)
                    new = kb[j, base + i] * around
                    if same is not None:
                        new = ab[j, base + i] * same[j] + new
                    row.append(new)
                nxt.append(row)
            return nxt

        def some(i, carry):
            groups_ = [together * i + k for k in range(together)]
            fields = []
            for r in range(4):
                for j in range(4):
                    for g in groups_:
                        theirs = edge[side, j, pl.ds(r * mf + 8 * g, 8), :]
                        fields.append(theirs * ceb[side, j, r])
            olds = [
                [[fields[(4 * r + j) * together + k] for j in range(4)] for r in range(4)]
                for k in range(together)
            ]
            for step in range(1, SPREAD_PASSES + 1):
                olds = [advance(old, step) for old in olds]
            for i in range(4):
                r = i + (4 if side == 0 else 8)
                for j in range(4):
                    total = acc[j, r + 4]
                    for old, g in zip(olds, groups_):
                        total = total + old[i][j] * mbuf[j, pl.ds(r * mf + 8 * g, 8), :]
                    acc[j, r + 4] = total
            return carry

        lax.fori_loop(0, steps // together, some, 0)

    spans = [(0, 32), (64, 96), (32, 64)]
    shares = []
    for low, high in spans[:2]:
        shares.append(
            [
                send(
                    part.at[lax.rem(m + o, groups), low:high], got.at[o - 1, low:high], o, 0,
                    start=False,
                )
                for o in (1, 2, 3)
            ]
        )
    shares.append(
        [
            send(part_x.at[lax.rem(m + o, groups)], got_x.at[o - 1], o, 0, start=False)
            for o in (1, 2, 3)
        ]
    )
    sub = lax.broadcasted_iota(jnp.int32, (4, 8, 128), 1)
    near32 = lax.broadcasted_iota(jnp.int32, (32, 128), 1) < 64

    def share(piece):
        low, high = spans[piece]
        folded = []
        for j in range(4):
            x = acc[j, low // 4 : high // 4]
            y = (x + pltpu.roll(x, 4, 1)).reshape(4, 2, 8, 128)
            folded.append(jnp.where(sub < 4, y[:, 0], y[:, 1]).reshape(32, 128))
        out = split_dot(jnp.concatenate(folded, axis=1), perm[...], transposed=True)
        quarters = [out[:, 128 * q : 128 * q + 128] for q in range(4)]
        for q in range(4):
            if piece < 2:
                part[q, low:high] = quarters[q]
            else:
                part_x[q, 0:32] = quarters[q]
                part_x[q, 32:64] = jnp.where(
                    near32, quarters[min(q + 1, 3)], quarters[max(q - 1, 0)]
                )
        for copy, _, _ in shares[piece]:
            copy.start()

    def finish(side):
        exists = there(0, 1 if side else -1)
        only(exists, functools.partial(meet_edge, side))
        share(side)
        only(exists, functools.partial(spread_edge, side))

    pl.when(~down_end)(functools.partial(finish, 0))
    finish(1)
    pl.when(down_end)(functools.partial(finish, 0))
    share(2)

    wait_all(rim_table)
    wait_all(rim_scale)
    near = lax.broadcasted_iota(jnp.int32, (16, 128), 1) < 64
    side_on = jnp.where(near, (m < groups - 1).astype(jnp.int32), (m > 0).astype(jnp.int32)) > 0
    for a in range(4):
        both = jnp.where(near, table_col_in[1, a], table_col_in[0, a])
        table_h[a, 8:24] = jnp.where(side_on, both, 0.0)
    near1 = near[0:1]
    for side, first in ((0, 12), (1, 0)):
        on = (t > 0) if side == 0 else (t < tiles - 1)
        row = 7 if side == 0 else 24
        for b in range(4):
            table[first + b, row : row + 1] = jnp.where(on, scale_in[side, 16 + b : 17 + b, 128:256], 0.0)
        both = jnp.where(near1, scale_in[side, 16:17, 384:512], scale_in[side, 19:20, 0:128])
        table_h[first // 4, row : row + 1] = jnp.where(side_on[0:1] & on, both, 0.0)

    rims = []
    for piece, (low, high) in enumerate(spans[:2]):
        wait_all(shares[piece])
        esum[1, low:high] = (part[m, low:high] + got[0, low:high]) + (
            got[1, low:high] + got[2, low:high]
        )
    for dm, dt in AROUND:
        slot = 1 - dm
        if dt == 0:
            for low, high in spans[:2]:
                rims.append(send_near(esum.at[1, low:high], esum.at[slot, low:high], dm, dt))
        elif dt == 1:
            rims.append(send_near(esum.at[1, 72:96], eup.at[slot], dm, dt))
        else:
            rims.append(send_near(esum.at[1, 0:24], edown.at[slot], dm, dt))

    fetch_rate.wait()
    unpack(scale_in, scale)
    for f in range(FIELDS):
        p = jnp.where(inside, rimmed(scale, f) * rimmed(grad, f), 0.0)
        for _ in range(STATIC_PASSES):
            around = (pltpu.roll(p, 1, 0) + pltpu.roll(p, 47, 0)) + (
                pltpu.roll(p, 1, 1) + pltpu.roll(p, 383, 1)
            )
            p = jnp.where(inside, p + rate_ref[f] * (around - 4.0 * p), 0.0)
        static_ref[f] = scale[f, 8:40, 128:384] * p[8:40, 0:256]

    wait_all(shares[2])
    far = (part_x[m] + got_x[0]) + (got_x[1] + got_x[2])
    esum[1, 32:64] = far[0:32]
    wait_all(rims)
    members_all = member_count * groups

    def whole(slot):
        for low, high in spans if slot == 1 else spans[:2]:
            eall[slot, low:high] = esum[slot, low:high]
        eall[slot, 8:32] += eup[slot]
        eall[slot, 64:88] += edown[slot]

    for slot in range(3):
        whole(slot)
    lane96 = lax.broadcasted_iota(jnp.int32, (96, 128), 1)
    side_e = jnp.where(lane96 < 64, eall[2], eall[0]) / (members_all - 1)
    eall[1] = eall[1] / (members_all - 1)
    eall[0] = side_e
    eall[0, 32:64] = far[32:64] / (members_all - 1)
    for parity in range(2):
        pairs = [(1, 0), (3, -1)] if parity == 0 else [(2, 0), (0, 1)]
        for f in range(FIELDS):
            at_row = 16 * (4 * parity + f)
            mids = [eall[1, pl.ds(4 * (4 + d) + f, 16, stride=4), :] for _, d in pairs]
            ends = [eall[0, pl.ds(4 * (4 + d) + f, 16, stride=4), :] for _, d in pairs]
            for b in range(4):
                lhs[at_row : at_row + 16, 128 * b : 128 * b + 128] = (
                    table[4 * pairs[0][0] + b, 8:24] * mids[0]
                    + table[4 * pairs[1][0] + b, 8 + pairs[1][1] : 24 + pairs[1][1]] * mids[1]
                )
            lhs[at_row : at_row + 16, 512:640] = (
                table_h[pairs[0][0], 8:24] * ends[0]
                + table_h[pairs[1][0], 8 + pairs[1][1] : 24 + pairs[1][1]] * ends[1]
            )
    out = split_dot(lhs[...], place[...])
    for parity in range(2):
        for f in range(FIELDS):
            at_row = 16 * (4 * parity + f)
            for x in range(2):
                fine[x, pl.ds(32 * f + parity, 16, stride=2), :] = out[
                    at_row : at_row + 16, 128 * x : 128 * x + 128
                ]
    for f in range(FIELDS):
        for x in range(2):
            cols = slice(128 * x, 128 * x + 128)
            fine_ref[f, :, cols] = fine[x, 32 * f : 32 * f + 32]
    for copy, going, _ in sent:
        only(going, copy.wait_send)


def local(gradient, static_scale, static_rate, interp_index, interp_weight, members, spread_rate):
    member_count = members.shape[0]
    mf = member_count * FIELDS
    anywhere = pl.BlockSpec(memory_space=pl.ANY)
    vmem = pltpu.VMEM
    sems = 54
    static, fine = pl.pallas_call(
        kernel,
        out_shape=[jax.ShapeDtypeStruct(gradient.shape, F32)] * 2,
        in_specs=[anywhere] * 7,
        out_specs=[pl.BlockSpec(memory_space=pltpu.VMEM)] * 2,
        scratch_shapes=[
            vmem((4, 48, 512), F32),
            vmem((4, 48, 512), F32),
            vmem((2, 16, 256), F32),
            vmem((2, 16, 512), F32),
            vmem((2, 24, 256), F32),
            vmem((2, 24, 512), F32),
            vmem((4, 16, 128), jnp.int32),
            vmem((4, 16, 128), F32),
            vmem((2, 4, 16, 128), F32),
            vmem((2, 4, 16, 128), F32),
            vmem((32, 512), F32),
            vmem(members.shape, BF16),
            vmem((512, 512), BF16),
            vmem((384, 512), BF16),
            vmem((640, 256), BF16),
            vmem((4, 16 * mf, 128), F32),
            vmem((2, 4, 4 * mf, 128), F32),
            vmem((4, 2 * mf, 128), F32),
            vmem((16, 32, 128), F32),
            vmem((4, 32, 128), F32),
            vmem((4, 192, 128), F32),
            vmem((4, 4, 16, 128), F32),
            vmem((2, 4, 16, 128), F32),
            vmem((2, 4, 16, 128), F32),
            vmem((4, 64, 128), F32),
            vmem((4, 16, 8, 128), F32),
            vmem((2, 4, 4, 8, 128), F32),
            vmem((4, 32, 8, 128), F32),
            vmem((4, 32, 8, 128), F32),
            vmem((2, 4, 32, 8, 128), F32),
            vmem((2, 4, 32, 8, 128), F32),
            vmem((4, 24, 8, 128), F32),
            vmem((mf // 8, 4, 8, 8, 128), F32),
            vmem((4, 96, 128), F32),
            vmem((4, 64, 128), F32),
            vmem((3, 96, 128), F32),
            vmem((3, 64, 128), F32),
            vmem((3, 96, 128), F32),
            vmem((3, 24, 128), F32),
            vmem((3, 24, 128), F32),
            vmem((3, 96, 128), F32),
            vmem((128, 640), F32),
            vmem((2, 128, 128), F32),
            pltpu.SMEM((4,), F32),
            pltpu.SemaphoreType.DMA((7,)),
            pltpu.SemaphoreType.DMA((sems,)),
            pltpu.SemaphoreType.DMA((sems,)),
        ],
        compiler_params=pltpu.CompilerParams(
            collective_id=0, has_side_effects=True, vmem_limit_bytes=18 << 20
        ),
    )(*[pltpu.with_memory_space_constraint(x, pltpu.HBM) for x in (static_rate, gradient, static_scale, interp_index, interp_weight, members, spread_rate)])
    return 0.3 * static + 2.8 * fine


def solution(mesh):
    return jax.shard_map(
        local,
        mesh=mesh,
        in_specs=(
            P(None, "tile", "mem"),
            P(None, "tile", "mem"),
            P(),
            P(None, "tile", "mem"),
            P(None, "tile", "mem"),
            P("mem", None, "tile", None),
            P("tile", None),
        ),
        out_specs=P(None, "tile", "mem"),
        check_vma=False,
    )
```

```python
import functools

import jax
import jax.numpy as jnp
from jax import lax
from jax.experimental import pallas as pl
from jax.experimental.pallas import tpu as pltpu
from jax.sharding import PartitionSpec as P

STATIC_PASSES = 4
SPREAD_PASSES = 8
REACH = SPREAD_PASSES // 2
FIELDS = 4
MESH = pl.DeviceIdType.MESH
F32 = jnp.float32
BF16 = jnp.bfloat16
AROUND = [(0, 1), (0, -1), (1, 0), (-1, 0), (1, 1), (1, -1), (-1, 1), (-1, -1)]
ZROW = 16
SENDS = 41


def split_dot(x, one_hot, transposed=False):
    high = x.astype(BF16)
    rest = x - high.astype(F32)
    mid = rest.astype(BF16)
    low = (rest - mid.astype(F32)).astype(BF16)
    terms = jnp.concatenate([high, mid, low], axis=0)
    dims = (((1,), (1 if transposed else 0,)), ((), ()))
    out = lax.dot_general(terms, one_hot, dims, preferred_element_type=F32)
    n = x.shape[0]
    return (out[2 * n :] + out[n : 2 * n]) + out[:n]


def first_row(step):
    return max(-step, step - SPREAD_PASSES - REACH)


def beside(row, lane):
    axis = row[0].ndim - 1
    zero = jnp.zeros_like(row[0])
    left = jnp.where(lane == 0, zero, pltpu.roll(row[3], 1, axis))
    right = jnp.where(lane == 127, zero, pltpu.roll(row[0], 127, axis))
    return [left + row[1], row[0] + row[2], row[1] + row[3], row[2] + right]


def kernel(
    rate_hbm, grad_hbm, scale_hbm, index_hbm, weight_hbm, members_hbm, spread_hbm, static_ref, fine_ref,
    grad, scale, grad_out, grad_in, scale_out, scale_in, index, weight,
    table_col, table_col_in, spread, raw, perm, pick, place,
    mbuf, edge, passing, table, table_h, picked, coarse, coarse_out, coarse_e, cperm, cb, ceb, kb, ab,
    pa, pb, acc, halo_v, part, part_x, got, got_x, esum, eup, edown, eall, lhs, fine,
    rate_ref, local_sem, send_sem, recv_sem,
):
    m, t = lax.axis_index("mem"), lax.axis_index("tile")
    groups, tiles = lax.axis_size("mem"), lax.axis_size("tile")
    member_count = raw.shape[0]
    mf = member_count * FIELDS
    steps = mf // 8

    def at(dm, dt):
        return (lax.rem(m + dm + groups, groups), lax.rem(t + dt + tiles, tiles))

    def there(dm, dt):
        tests = []
        if dm:
            tests.append(m < groups - 1 if dm > 0 else m > 0)
        if dt:
            tests.append(t < tiles - 1 if dt > 0 else t > 0)
        return functools.reduce(jnp.logical_and, tests) if tests else None

    def only(test, action):
        if test is None:
            action()
        else:
            pl.when(test)(action)

    barrier = pltpu.get_barrier_semaphore()

    def greet(dm, dt):
        pl.semaphore_signal(barrier, inc=1, device_id=at(dm, dt), device_id_type=MESH)

    waited = 3
    for o in (1, 2, 3):
        greet(o, 0)
    for dm, dt in AROUND:
        if dt:
            only(there(dm, dt), functools.partial(greet, dm, dt))
            waited = waited + there(dm, dt).astype(jnp.int32)
    up_end, down_end = lax.rem(t, ZROW) == ZROW - 1, lax.rem(t, ZROW) == 0
    feeder = (up_end & (t < tiles - 1)) | (down_end & (t > 0))
    relay = (up_end | down_end) & ~feeder
    over = jnp.where(t < ZROW, ZROW, -ZROW)
    along = jnp.where(up_end, 1 - ZROW, ZROW - 1)

    @pl.when(up_end | down_end)
    def _():
        greet(0, over)
        greet(0, along)

    waited = waited + 2 * (up_end | down_end).astype(jnp.int32)

    locals_ = []

    def fetch(src, dst):
        copy = pltpu.make_async_copy(src, dst, local_sem.at[len(locals_)])
        locals_.append(copy)
        copy.start()
        return copy

    fetch_grad = fetch(grad_hbm, grad.at[:, 8:40, 128:384])
    fetch_members = fetch(members_hbm, raw)
    fetch_index = fetch(index_hbm, index)
    fetch_weight = fetch(weight_hbm, weight)
    fetch_spread = fetch(spread_hbm, spread.at[8:24])
    fetch_rate = fetch(rate_hbm, rate_ref)
    fetch_scale = fetch(scale_hbm, scale.at[:, 8:40, 128:384])

    sent = []
    slots, arrivals, slot_of = list(range(SENDS)), [], {}

    def send(src, dst, dm, dt, going=None, coming=None, start=True):
        number = slots.pop(0)
        arrivals.append(number)
        copy = pltpu.make_async_remote_copy(
            src_ref=src, dst_ref=dst, send_sem=send_sem.at[number], recv_sem=recv_sem.at[len(arrivals) - 1],
            device_id=at(dm, dt), device_id_type=MESH,
        )
        entry = (copy, going, coming)
        slot_of[id(copy)] = number
        sent.append(entry)
        if start:
            only(entry[1], copy.start)
        return entry

    def release(entries):
        for entry in entries:
            only(entry[1], entry[0].wait_send)
            slots.insert(0, slot_of[id(entry[0])])
        sent[:] = [kept for kept in sent if all(kept is not entry for entry in entries)]

    def send_near(src, dst, dm, dt):
        return send(src, dst, dm, dt, there(dm, dt), there(-dm, -dt))

    def pack(buf, out):
        for f in range(FIELDS):
            out[0, 4 * f : 4 * f + 4] = buf[f, 8:12, 128:384]
            out[1, 4 * f : 4 * f + 4] = buf[f, 36:40, 128:384]

    def send_rim(buf, out, come):
        copies = []
        for dm, dt in AROUND:
            col = {0: (128, 128, 256), 1: (256, 0, 128), -1: (128, 384, 128)}[dm]
            here, land = pl.ds(col[0], col[2]), pl.ds(col[1], col[2])
            if dt == 0:
                src, dst = buf.at[:, 8:40, here], buf.at[:, 8:40, land]
            else:
                side = 1 if dt > 0 else 0
                src = out.at[side, :, pl.ds(col[0] - 128, col[2])]
                dst = come.at[1 - side, :, land]
            copies.append(send_near(src, dst, dm, dt))
        return copies

    def unpack(come, buf):
        for f in range(FIELDS):
            buf[f, 4:8] = come[0, 4 * f : 4 * f + 4]
            buf[f, 40:44] = come[1, 4 * f : 4 * f + 4]

    def wait_all(copies):
        for copy, _, coming in copies:
            only(coming, copy.wait_recv)

    source = lax.broadcasted_iota(jnp.int32, (512, 512), 0)
    target = lax.broadcasted_iota(jnp.int32, (512, 512), 1)
    perm[...] = (source == 4 * (target & 127) + (target >> 7)).astype(F32).astype(BF16)

    fetch_members.wait()

    half = member_count // 2

    def convert(i):
        block = raw[half * i : half * i + half].reshape(half * FIELDS * 16, 512)
        for j in range(0, 4, 2):
            out = jnp.dot(
                block, perm[:, 128 * j : 128 * j + 256], preferred_element_type=F32
            )
            for q in range(half * FIELDS):
                for k in range(2):
                    mbuf[j + k, pl.ds(half * FIELDS * i + q, 16, stride=mf), :] = out[
                        16 * q : 16 * q + 16, 128 * k : 128 * k + 128
                    ]

    convert(0)
    convert(1)
    fetch_grad.wait()
    pack(grad, grad_out)
    fetch_spread.wait()
    pl.semaphore_wait(barrier, waited)
    rim_grad = send_rim(grad, grad_out, grad_in)
    rim_spread = [
        send_near(spread.at[16:24], spread.at[0:8], 0, 1),
        send_near(spread.at[8:16], spread.at[24:32], 0, -1),
    ]

    edge_members, late = [[], []], []
    for rows in (range(0, 2), range(2, 4)):
        first, count = rows[0] * mf, len(rows) * mf
        for side, dt, cross, crossed in ((0, 1, up_end, down_end), (1, -1, down_end, up_end)):
            here = pl.ds(first + (12 * mf if side == 0 else 0), count)
            going, coming = there(0, dt), there(0, -dt)
            if rows[0] == 0:
                going, coming = going & ~cross, coming & ~crossed
            entry = send(
                mbuf.at[:, here], edge.at[side, :, pl.ds(first, count)], 0, dt, going, coming,
                start=False,
            )
            edge_members[side].append(entry)
            only(going & ~cross, entry[0].start)
            if rows[0] == 2:
                late.append((going & cross, entry[0]))
    origin = jnp.where(up_end, 12 * mf, 0)
    over_z, onward = [], []
    middle = mf + mf // 16 * 8
    for low, high in ((0, mf), (mf, middle), (middle, 2 * mf)):
        from_row = pl.ds(pl.multiple_of(origin + low, 8), high - low)
        rows = pl.ds(low, high - low)
        over_z.append(
            send(mbuf.at[:, from_row], passing.at[:, rows], 0, over, feeder, relay, start=low == 0)
        )
        onward.append(
            send(
                passing.at[:, rows], edge.at[down_end.astype(jnp.int32), :, rows],
                0, along, relay, feeder, start=False,
            )
        )
    late += [(feeder, copy) for copy, _, _ in over_z[1:]]

    fetch_index.wait()
    fetch_weight.wait()
    for o in range(16):
        total = jnp.zeros((16, 128), F32)
        for s in range(4):
            total = total + jnp.where(index[s] == o, weight[s], 0.0)
        table[o, 8:24] = total
        if o % 4 in (0, 3):
            table_col[o % 4 // 3, o // 4] = total
        for x in (0, 128):
            if o < 4:
                scale_out[0, 16 + o : 17 + o, x : x + 128] = total[0:1]
            if o >= 12:
                scale_out[1, 4 + o : 5 + o, x : x + 128] = total[15:16]
    fetch_scale.wait()
    pack(scale, scale_out)
    source = lax.broadcasted_iota(jnp.int32, (384, 512), 0)
    target = lax.broadcasted_iota(jnp.int32, (384, 512), 1)
    wanted = 2 * (target & 127) + (target >> 7) - 1
    wanted = jnp.where(wanted < 0, 383, wanted)
    pick[...] = (source == wanted).astype(F32).astype(BF16)
    source = lax.broadcasted_iota(jnp.int32, (640, 256), 0)
    target = lax.broadcasted_iota(jnp.int32, (640, 256), 1)
    inner = (source < 512) & (target == 2 * (source & 127) + (source >> 7) - 1)
    left = (source == 639) & (target == 0)
    right = (source == 512) & (target == 255)
    place[...] = (inner | left | right).astype(F32).astype(BF16)

    rows48 = lax.broadcasted_iota(jnp.int32, (48, 384), 0)
    lanes48 = lax.broadcasted_iota(jnp.int32, (48, 384), 1)
    inside = (t > 0) | (rows48 >= 8)
    inside = inside & ((t < tiles - 1) | (rows48 < 40))
    inside = inside & ((m > 0) | (lanes48 < 320))
    inside = inside & ((m < groups - 1) | (lanes48 < 256) | (lanes48 >= 320))
    lane48 = lax.broadcasted_iota(jnp.int32, (48, 128), 1)

    def rimmed(buf, f):
        rim = jnp.where(lane48 < 64, buf[f, :, 384:512], buf[f, :, 0:128])
        return jnp.concatenate([buf[f, :, 128:384], rim], axis=1)

    wait_all(rim_grad)
    unpack(grad_in, grad)
    padded = jnp.concatenate(
        [jnp.where(inside, rimmed(grad, f), 0.0) for f in range(FIELDS)], axis=0
    )
    out = split_dot(padded, pick[...])
    for b in range(4):
        picked[b] = out[:, 128 * b : 128 * b + 128]
    for f in range(FIELDS):
        total = jnp.zeros((16, 128), F32)
        for a in range(4):
            for b in range(4):
                total = total + table[4 * a + b, 8:24] * picked[
                    b, pl.ds(48 * f + 7 + a, 16, stride=2), :
                ]
        coarse[m, f] = total
    all_coarse = [send(coarse.at[m], coarse.at[m], o, 0) for o in (1, 2, 3)]
    for test, copy in late:
        only(test, copy.start)

    wait_all(rim_spread)
    out = split_dot(spread[...], perm[...])
    row32 = lax.broadcasted_iota(jnp.int32, (32, 512), 0)
    known = ((t > 0) | (row32 >= 8)) & ((t < tiles - 1) | (row32 < 24))
    rate = jnp.where(known, out, 0.0)
    stay = jnp.where(known, 1.0 - 4.0 * out, 0.0)
    for j in range(4):
        for r in range(1, 31):
            kb[j, r] = jnp.broadcast_to(rate[r : r + 1, 128 * j : 128 * j + 128], (8, 128))
            ab[j, r] = jnp.broadcast_to(stay[r : r + 1, 128 * j : 128 * j + 128], (8, 128))
    acc[...] = jnp.zeros_like(acc)

    for side, dt in ((0, -1), (1, 1)):
        @pl.when(jnp.logical_not(there(0, dt)))
        def _():
            edge[side] = jnp.zeros_like(edge[side])

    for slot in range(3):
        for dt in (-1, 0, 1):
            if slot == 1 and dt == 0:
                continue
            dst = {-1: eup, 0: esum, 1: edown}[dt]

            @pl.when(jnp.logical_not(there(slot - 1, dt)))
            def _():
                dst[slot] = jnp.zeros_like(dst[slot])

    def pass_on(row):
        @pl.when(relay)
        def _():
            over_z[row][0].wait_recv()
            onward[row][0].start()

    wait_all(all_coarse)
    pass_on(0)
    for q in range(4):
        for f in range(FIELDS):
            coarse_out[0, q, 4 * f : 4 * f + 4] = coarse[q, f, 0:4]
            coarse_out[1, q, 4 * f : 4 * f + 4] = coarse[q, f, 12:16]
    release(rim_grad + rim_spread + all_coarse)
    edge_coarse = [
        send_near(coarse_out.at[1], coarse_e.at[0], 0, 1),
        send_near(coarse_out.at[0], coarse_e.at[1], 0, -1),
    ]
    rim_scale = send_rim(scale, scale_out, scale_in)
    rim_table = []
    for dm, dt in AROUND:
        if dt == 0:
            side = 1 if dm > 0 else 0
            rim_table.append(send_near(table_col.at[side], table_col_in.at[1 - side], dm, dt))

    rows = jnp.concatenate([coarse[q].reshape(64, 128) for q in range(4)], axis=1)
    out = split_dot(rows, perm[...])
    for j in range(4):
        cperm[j, 0:64] = out[:, 128 * j : 128 * j + 128]
    for j in range(4):
        for r in range(16):
            four = cperm[j, pl.ds(r, 4, stride=16), :]
            cb[j, r, 0:4] = four
            cb[j, r, 4:8] = four

    lane8 = lax.broadcasted_iota(jnp.int32, (8, 128), 1)
    together = 2 if steps % 2 == 0 else 1

    def spread_own(i, carry):
        for piece, when in ((1, 1), (2, 3)):
            @pl.when(i == min(when, steps // together - 1))
            def _():
                pass_on(piece)

        taken = [together * i + k for k in range(together)]
        for r in range(16):
            for j in range(4):
                c = cb[j, r]
                for k, g in enumerate(taken):
                    pa[k, j, r + 8] = mbuf[j, pl.ds(r * mf + 8 * g, 8), :] * c
        filled = (0, 15)
        for step in range(1, SPREAD_PASSES + 1):
            src, dst = (pa, pb) if step % 2 else (pb, pa)

            def line(k, r):
                if not filled[0] <= r <= filled[1]:
                    return None
                return [src[k, j, r + 8] for j in range(4)]

            low = first_row(step)
            high = 15 - low
            above = [line(k, low - 1) for k in range(together)]
            here = [line(k, low) for k in range(together)]
            for r in range(low, high + 1):
                below = [line(k, r + 1) for k in range(together)]
                rate_r = [kb[j, r + 8] for j in range(4)]
                stay_r = [ab[j, r + 8] for j in range(4)] if here[0] is not None else None
                for k, g in enumerate(taken):
                    sides = beside(here[k], lane8) if stay_r is not None else None
                    for j in range(4):
                        parts = [row[k][j] for row in (above, below) if row[k] is not None]
                        if sides is not None:
                            parts.append(sides[j])
                        new = rate_r[j] * functools.reduce(lambda a, b: a + b, parts)
                        if stay_r is not None:
                            new = stay_r[j] * here[k][j] + new
                        if step < SPREAD_PASSES:
                            dst[k, j, r + 8] = new
                        elif r < 0:
                            halo_v[g, j, r + 4] = new
                        elif r >= 16:
                            halo_v[g, j, r - 12] = new
                        else:
                            acc[j, r + 4] += new * mbuf[j, pl.ds(r * mf + 8 * g, 8), :]
                above, here = here, below
            filled = (low, high)
        return carry

    lax.fori_loop(0, steps // together, spread_own, 0)

    wait_all(edge_coarse)
    rows = jnp.concatenate(
        [
            jnp.concatenate([coarse_e[side, q] for q in range(4)], axis=1)
            for side in range(2)
        ],
        axis=0,
    )
    out = split_dot(rows, perm[...])
    for j in range(4):
        cperm[j, 0:32] = out[:, 128 * j : 128 * j + 128]
    for side in range(2):
        known = (t > 0) if side == 0 else (t < tiles - 1)
        for j in range(4):
            for r in range(4):
                four = jnp.where(known, cperm[j, pl.ds(16 * side + r, 4, stride=4), :], 0.0)
                ceb[side, j, r, 0:4] = four
                ceb[side, j, r, 4:8] = four
    def meet_edge(side):
        wait_all(edge_members[side])
        for copy, _, _ in onward:
            only(down_end & feeder if side == 0 else up_end & feeder, copy.wait_recv)

        for r in range(4):
            for j in range(4):
                terms = [
                    edge[side, j, pl.ds(r * mf + 8 * g, 8), :] * halo_v[g, j, 4 * side + r]
                    for g in range(steps)
                ]
                acc[j, r if side == 0 else 20 + r] = functools.reduce(lambda a, b: a + b, terms)

    def spread_edge(side):
        def advance(old, step):
            base = 8 + (step - REACH if side == 0 else 16 - step)
            shift = 1 if side == 0 else -1
            nxt = []
            for i in range(4):
                terms = [old[i + shift + d] for d in (-1, 1) if 0 <= i + shift + d < 4]
                row = []
                same = old[i + shift] if 0 <= i + shift < 4 else None
                sides = beside(same, lane8) if same is not None else None
                for j in range(4):
                    parts = [term[j] for term in terms]
                    if sides is not None:
                        parts.append(sides[j])
                    around = functools.reduce(lambda a, b: a + b, parts)
                    new = kb[j, base + i] * around
                    if same is not None:
                        new = ab[j, base + i] * same[j] + new
                    row.append(new)
                nxt.append(row)
            return nxt

        def some(i, carry):
            groups_ = [together * i + k for k in range(together)]
            fields = []
            for r in range(4):
                for j in range(4):
                    for g in groups_:
                        theirs = edge[side, j, pl.ds(r * mf + 8 * g, 8), :]
                        fields.append(theirs * ceb[side, j, r])
            olds = [
                [[fields[(4 * r + j) * together + k] for j in range(4)] for r in range(4)]
                for k in range(together)
            ]
            for step in range(1, SPREAD_PASSES + 1):
                olds = [advance(old, step) for old in olds]
            for i in range(4):
                r = i + (4 if side == 0 else 8)
                for j in range(4):
                    total = acc[j, r + 4]
                    for old, g in zip(olds, groups_):
                        total = total + old[i][j] * mbuf[j, pl.ds(r * mf + 8 * g, 8), :]
                    acc[j, r + 4] = total
            return carry

        lax.fori_loop(0, steps // together, some, 0)

    spans = [(0, 32), (64, 96), (32, 64)]
    shares = []
    for low, high in spans[:2]:
        shares.append(
            [
                send(
                    part.at[lax.rem(m + o, groups), low:high], got.at[o - 1, low:high], o, 0,
                    start=False,
                )
                for o in (1, 2, 3)
            ]
        )
    shares.append(
        [
            send(part_x.at[lax.rem(m + o, groups)], got_x.at[o - 1], o, 0, start=False)
            for o in (1, 2, 3)
        ]
    )
    sub = lax.broadcasted_iota(jnp.int32, (4, 8, 128), 1)
    near32 = lax.broadcasted_iota(jnp.int32, (32, 128), 1) < 64

    def share(piece):
        low, high = spans[piece]
        folded = []
        for j in range(4):
            x = acc[j, low // 4 : high // 4]
            y = (x + pltpu.roll(x, 4, 1)).reshape(4, 2, 8, 128)
            folded.append(jnp.where(sub < 4, y[:, 0], y[:, 1]).reshape(32, 128))
        out = split_dot(jnp.concatenate(folded, axis=1), perm[...], transposed=True)
        quarters = [out[:, 128 * q : 128 * q + 128] for q in range(4)]
        for q in range(4):
            if piece < 2:
                part[q, low:high] = quarters[q]
            else:
                part_x[q, 0:32] = quarters[q]
                part_x[q, 32:64] = jnp.where(
                    near32, quarters[min(q + 1, 3)], quarters[max(q - 1, 0)]
                )
        for copy, _, _ in shares[piece]:
            copy.start()

    def finish(side):
        exists = there(0, 1 if side else -1)
        only(exists, functools.partial(meet_edge, side))
        share(side)
        only(exists, functools.partial(spread_edge, side))

    pl.when(~down_end)(functools.partial(finish, 0))
    finish(1)
    pl.when(down_end)(functools.partial(finish, 0))
    share(2)

    wait_all(rim_table)
    wait_all(rim_scale)
    near = lax.broadcasted_iota(jnp.int32, (16, 128), 1) < 64
    side_on = jnp.where(near, (m < groups - 1).astype(jnp.int32), (m > 0).astype(jnp.int32)) > 0
    for a in range(4):
        both = jnp.where(near, table_col_in[1, a], table_col_in[0, a])
        table_h[a, 8:24] = jnp.where(side_on, both, 0.0)
    near1 = near[0:1]
    for side, first in ((0, 12), (1, 0)):
        on = (t > 0) if side == 0 else (t < tiles - 1)
        row = 7 if side == 0 else 24
        for b in range(4):
            table[first + b, row : row + 1] = jnp.where(on, scale_in[side, 16 + b : 17 + b, 128:256], 0.0)
        both = jnp.where(near1, scale_in[side, 16:17, 384:512], scale_in[side, 19:20, 0:128])
        table_h[first // 4, row : row + 1] = jnp.where(side_on[0:1] & on, both, 0.0)

    rims = []
    for piece, (low, high) in enumerate(spans[:2]):
        wait_all(shares[piece])
        esum[1, low:high] = (part[m, low:high] + got[0, low:high]) + (
            got[1, low:high] + got[2, low:high]
        )
    for dm, dt in AROUND:
        slot = 1 - dm
        if dt == 0:
            for low, high in spans[:2]:
                rims.append(send_near(esum.at[1, low:high], esum.at[slot, low:high], dm, dt))
        elif dt == 1:
            rims.append(send_near(esum.at[1, 72:96], eup.at[slot], dm, dt))
        else:
            rims.append(send_near(esum.at[1, 0:24], edown.at[slot], dm, dt))

    fetch_rate.wait()
    unpack(scale_in, scale)
    for f in range(FIELDS):
        p = jnp.where(inside, rimmed(scale, f) * rimmed(grad, f), 0.0)
        for _ in range(STATIC_PASSES):
            around = (pltpu.roll(p, 1, 0) + pltpu.roll(p, 47, 0)) + (
                pltpu.roll(p, 1, 1) + pltpu.roll(p, 383, 1)
            )
            p = jnp.where(inside, p + rate_ref[f] * (around - 4.0 * p), 0.0)
        static_ref[f] = scale[f, 8:40, 128:384] * p[8:40, 0:256]

    wait_all(shares[2])
    far = (part_x[m] + got_x[0]) + (got_x[1] + got_x[2])
    esum[1, 32:64] = far[0:32]
    wait_all(rims)
    members_all = member_count * groups

    def whole(slot):
        for low, high in spans if slot == 1 else spans[:2]:
            eall[slot, low:high] = esum[slot, low:high]
        eall[slot, 8:32] += eup[slot]
        eall[slot, 64:88] += edown[slot]

    for slot in range(3):
        whole(slot)
    lane96 = lax.broadcasted_iota(jnp.int32, (96, 128), 1)
    side_e = jnp.where(lane96 < 64, eall[2], eall[0]) / (members_all - 1)
    eall[1] = eall[1] / (members_all - 1)
    eall[0] = side_e
    eall[0, 32:64] = far[32:64] / (members_all - 1)
    for parity in range(2):
        pairs = [(1, 0), (3, -1)] if parity == 0 else [(2, 0), (0, 1)]
        for f in range(FIELDS):
            at_row = 16 * (4 * parity + f)
            mids = [eall[1, pl.ds(4 * (4 + d) + f, 16, stride=4), :] for _, d in pairs]
            ends = [eall[0, pl.ds(4 * (4 + d) + f, 16, stride=4), :] for _, d in pairs]
            for b in range(4):
                lhs[at_row : at_row + 16, 128 * b : 128 * b + 128] = (
                    table[4 * pairs[0][0] + b, 8:24] * mids[0]
                    + table[4 * pairs[1][0] + b, 8 + pairs[1][1] : 24 + pairs[1][1]] * mids[1]
                )
            lhs[at_row : at_row + 16, 512:640] = (
                table_h[pairs[0][0], 8:24] * ends[0]
                + table_h[pairs[1][0], 8 + pairs[1][1] : 24 + pairs[1][1]] * ends[1]
            )
    out = split_dot(lhs[...], place[...])
    for parity in range(2):
        for f in range(FIELDS):
            at_row = 16 * (4 * parity + f)
            for x in range(2):
                fine[x, pl.ds(32 * f + parity, 16, stride=2), :] = out[
                    at_row : at_row + 16, 128 * x : 128 * x + 128
                ]
    for f in range(FIELDS):
        for x in range(2):
            cols = slice(128 * x, 128 * x + 128)
            fine_ref[f, :, cols] = fine[x, 32 * f : 32 * f + 32]
    for copy, going, _ in sent:
        only(going, copy.wait_send)


def local(gradient, static_scale, static_rate, interp_index, interp_weight, members, spread_rate):
    member_count = members.shape[0]
    mf = member_count * FIELDS
    anywhere = pl.BlockSpec(memory_space=pl.ANY)
    vmem = pltpu.VMEM
    static, fine = pl.pallas_call(
        kernel,
        out_shape=[jax.ShapeDtypeStruct(gradient.shape, F32)] * 2,
        in_specs=[anywhere] * 7,
        out_specs=[pl.BlockSpec(memory_space=pltpu.VMEM)] * 2,
        scratch_shapes=[
            vmem((4, 48, 512), F32),
            vmem((4, 48, 512), F32),
            vmem((2, 16, 256), F32),
            vmem((2, 16, 512), F32),
            vmem((2, 24, 256), F32),
            vmem((2, 24, 512), F32),
            vmem((4, 16, 128), jnp.int32),
            vmem((4, 16, 128), F32),
            vmem((2, 4, 16, 128), F32),
            vmem((2, 4, 16, 128), F32),
            vmem((32, 512), F32),
            vmem(members.shape, BF16),
            vmem((512, 512), BF16),
            vmem((384, 512), BF16),
            vmem((640, 256), BF16),
            vmem((4, 16 * mf, 128), F32),
            vmem((2, 4, 4 * mf, 128), F32),
            vmem((4, 2 * mf, 128), F32),
            vmem((16, 32, 128), F32),
            vmem((4, 32, 128), F32),
            vmem((4, 192, 128), F32),
            vmem((4, 4, 16, 128), F32),
            vmem((2, 4, 16, 128), F32),
            vmem((2, 4, 16, 128), F32),
            vmem((4, 64, 128), F32),
            vmem((4, 16, 8, 128), F32),
            vmem((2, 4, 4, 8, 128), F32),
            vmem((4, 32, 8, 128), F32),
            vmem((4, 32, 8, 128), F32),
            vmem((2, 4, 32, 8, 128), F32),
            vmem((2, 4, 32, 8, 128), F32),
            vmem((4, 24, 8, 128), F32),
            vmem((mf // 8, 4, 8, 8, 128), F32),
            vmem((4, 96, 128), F32),
            vmem((4, 64, 128), F32),
            vmem((3, 96, 128), F32),
            vmem((3, 64, 128), F32),
            vmem((3, 96, 128), F32),
            vmem((3, 24, 128), F32),
            vmem((3, 24, 128), F32),
            vmem((3, 96, 128), F32),
            vmem((128, 640), F32),
            vmem((2, 128, 128), F32),
            pltpu.SMEM((4,), F32),
            pltpu.SemaphoreType.DMA((7,)),
            pltpu.SemaphoreType.DMA((SENDS,)),
            pltpu.SemaphoreType.DMA((54,)),
        ],
        compiler_params=pltpu.CompilerParams(
            collective_id=0, has_side_effects=True, vmem_limit_bytes=18 << 20
        ),
    )(*[pltpu.with_memory_space_constraint(x, pltpu.HBM) for x in (static_rate, gradient, static_scale, interp_index, interp_weight, members, spread_rate)])
    return 0.3 * static + 2.8 * fine


def solution(mesh):
    return jax.shard_map(
        local,
        mesh=mesh,
        in_specs=(
            P(None, "tile", "mem"),
            P(None, "tile", "mem"),
            P(),
            P(None, "tile", "mem"),
            P(None, "tile", "mem"),
            P("mem", None, "tile", None),
            P("tile", None),
        ),
        out_specs=P(None, "tile", "mem"),
        check_vma=False,
    )
```
